32 devices in a mesh: inst: 2 (over x), qy: 4 (over z), qx: 4 (over y, core).
Axes of the slice: x: 2, y: 2, z: 4, core: 2. Of those that a mesh axis runs over, the one named last changes fastest.
Arguments:
- cost_diag: float32 [8388608], P(('inst', 'qx', 'qy')), parts along dimension 0
- gammas: float32 [6], replicated
- betas: float32 [6], replicated
Outputs:
- output 1: float32 [2], P('inst'), parts along dimension 0
- output 2: float32 [8388608], P(('inst', 'qx', 'qy')), parts along dimension 0
- output 3: float32 [8388608], P(('inst', 'qx', 'qy')), parts along dimension 0
There are 2 independent parts. The reference program is written for one: setup_inputs(seed, part) draws one part's arguments, and reference() takes and returns one part's arrays. A program takes and returns all parts, laid end to end along the dimension named above; an argument that names none is the same for every part.
All inputs are finite; a program needn't handle non-finite values.
Results may differ from the reference program's by a relative error of at most 0.001.
Values sent between devices are 32-bit elements.
A program may use at most 1 GiB of HBM per device.

```python
import math
import jax
import jax.numpy as jnp
from jax import lax

STATE = 4194304
LAYERS = 6
DEGREE = 8

QUBITS = int(math.log2(STATE))
EDGES = DEGREE * QUBITS // 2


def setup_inputs(seed: int = 0, part: int = 0) -> dict:
    base_key = jax.random.key(seed)
    part_key = jax.random.fold_in(base_key, part)
    key_offset, key_weight = jax.random.split(part_key)
    first_node = jnp.arange(EDGES, dtype=jnp.int32) % QUBITS
    offsets = jax.random.randint(key_offset, (EDGES,), 1, QUBITS, dtype=jnp.int32)
    second_node = (first_node + offsets) % QUBITS
    weights = jax.random.uniform(key_weight, (EDGES,), jnp.float32, 0.5, 1.5) * (2.0 / math.sqrt(EDGES))
    basis_index = jnp.arange(STATE, dtype=jnp.int32)

    def add_edge(edge_id, cost_acc):
        cut_bit = ((basis_index >> first_node[edge_id]) ^ (basis_index >> second_node[edge_id])) & 1
        return cost_acc + weights[edge_id] * cut_bit.astype(jnp.float32)

    cost_diag = lax.fori_loop(0, EDGES, add_edge, jnp.zeros((STATE,), jnp.float32))
    key_gamma, key_beta = jax.random.split(jax.random.key(seed + 1))
    gammas = jax.random.uniform(key_gamma, (LAYERS,), jnp.float32, 0.3, 1.0)
    betas = jax.random.uniform(key_beta, (LAYERS,), jnp.float32, 0.4, 1.2)
    return {'cost_diag': cost_diag, 'gammas': gammas, 'betas': betas}


def apply_mixer(state_re, state_im, cos_half, sin_half):
    for qubit_id in range(QUBITS):
        view_shape = (STATE >> (qubit_id + 1), 2, 1 << qubit_id)
        view_re = state_re.reshape(view_shape)
        view_im = state_im.reshape(view_shape)
        flip_re = jnp.flip(view_re, axis=1)
        flip_im = jnp.flip(view_im, axis=1)
        state_re = (cos_half * view_re + sin_half * flip_im).reshape(STATE)
        state_im = (cos_half * view_im - sin_half * flip_re).reshape(STATE)
    return state_re, state_im


def reference(cost_diag, gammas, betas):
    def layer_step(scan_carry, angles):
        state_re, state_im = scan_carry
        layer_gamma, layer_beta = angles
        phase_angle = layer_gamma * cost_diag
        cos_phase = jnp.cos(phase_angle)
        sin_phase = jnp.sin(phase_angle)
        new_re = state_re * cos_phase + state_im * sin_phase
        new_im = state_im * cos_phase - state_re * sin_phase
        cos_half = jnp.cos(0.5 * layer_beta)
        sin_half = jnp.sin(0.5 * layer_beta)
        return apply_mixer(new_re, new_im, cos_half, sin_half), None

    init_state = (jnp.ones((STATE,), jnp.float32), jnp.zeros((STATE,), jnp.float32))
    final_state, layer_outs = lax.scan(layer_step, init_state, (gammas, betas))
    state_re, state_im = final_state
    energy = jnp.sum(cost_diag * (state_re * state_re + state_im * state_im)) / STATE
    return energy.reshape(1), state_re, state_im
```

```python
import functools

import jax
import jax.numpy as jnp
from jax import lax
from jax.experimental import pallas as pl
from jax.experimental.pallas import tpu as pltpu
from jax.sharding import PartitionSpec as P

LANES = 128
SUBLANES = 8
BLOCKS = 16
CHUNKS = 8


def flip(x, m):
    return (x // 2 + m // 2) % 2 * 2 + (x + m) % 2


def rx_pair(a, b, c, s):
    (ar, ai), (br, bi) = a, b
    return (c * ar + s * bi, c * ai - s * br), (c * br + s * ai, c * bi - s * ar)


def rx_list(amps, c, s):
    amps = list(amps)
    step = 1
    while step < len(amps):
        for i in range(len(amps)):
            if not i & step:
                amps[i], amps[i + step] = rx_pair(amps[i], amps[i + step], c, s)
        step *= 2
    return amps


def kernel(layers, vregs, total, cost_in, gam, bet, en_out, re_out, im_out,
           cost, trig, recv, work, send, tabs, en_send, en_recv,
           load_sem, csend_sem, crecv_sem, send_sem, recv_sem, esend_sem, erecv_sem, store_sem):
    n = CHUNKS
    half = n // 2
    per = vregs // n
    a, b = lax.axis_index("qx"), lax.axis_index("qy")
    me = a * 4 + b

    def loop(lo, hi, body):
        def step(i, carry):
            body(i)
            return carry

        lax.fori_loop(lo, hi, step, 0)

    def peer(i):
        m = 15 - i
        pa, pb = flip(a, m % 4), flip(b, m // 4)
        return pa * 4 + pb, {"qx": pa, "qy": pb}

    def put(src, dst, send_s, recv_s, dev):
        return pltpu.make_async_remote_copy(src, dst, send_s, recv_s, device_id=dev,
                                            device_id_type=pl.DeviceIdType.MESH)

    def load(k):
        return pltpu.make_async_copy(cost_in.at[:, k], cost.at[0, k], load_sem.at[k])

    loop(0, n, lambda k: load(k).start())
    barrier = pltpu.get_barrier_semaphore()
    loop(0, 15, lambda i: pl.semaphore_signal(barrier, inc=1, device_id=peer(i)[1],
                                              device_id_type=pl.DeviceIdType.MESH))
    pl.semaphore_wait(barrier, 15)

    def share(k):
        load(k).wait()

        def one(i):
            j, dev = peer(i)
            put(cost.at[0, k, j], cost.at[1, k, me], csend_sem.at[k], crecv_sem.at[k], dev).start()

        loop(0, 15, one)
        pltpu.make_async_copy(cost.at[0, k, me], cost.at[1, k, me], crecv_sem.at[k]).start()

    loop(0, n, share)

    def tables(l):
        angle = jnp.full((SUBLANES, LANES), 0.5 * bet[l], jnp.float32)
        tabs[l, 0] = jnp.cos(angle)
        tabs[l, 1] = jnp.sin(angle)

    loop(0, layers, tables)

    def rows(v):
        return pl.ds(v * SUBLANES, SUBLANES)

    def angles(l, lay, k):
        g = gam[l]

        def body(i):
            for v in range(per):
                t = g * cost[lay, k, i, rows(v), :]
                trig[k, 0, i, rows(v), :] = jnp.cos(t)
                trig[k, 1, i, rows(v), :] = jnp.sin(t)

        loop(0, BLOCKS, body)

    def inner(buf, k, l):
        c, s = tabs[l, 0], tabs[l, 1]
        place = [lax.broadcasted_iota(jnp.int32, (SUBLANES, LANES), d) for d in range(2)]

        def partner(v, axis, step):
            size = (SUBLANES, LANES)[axis]
            if 2 * step == size:
                return pltpu.roll(v, step, axis)
            return jnp.where((place[axis] & step) != 0, pltpu.roll(v, step, axis), pltpu.roll(v, size - step, axis))

        def body(i):
            amps = []
            for v in range(per):
                re, im = buf[k, i, 0, rows(v), :], buf[k, i, 1, rows(v), :]
                for axis, bits in ((1, 7), (0, 3)):
                    for q in range(bits):
                        pr, pi = partner(re, axis, 1 << q), partner(im, axis, 1 << q)
                        re, im = c * re + s * pi, c * im - s * pr
                amps.append((re, im))
            for v, (re, im) in enumerate(rx_list(amps, c, s)):
                buf[k, i, 0, rows(v), :] = re
                buf[k, i, 1, rows(v), :] = im

        loop(0, BLOCKS, body)

    def block_bits(l, k, get, dst):
        c, s = tabs[l, 0], tabs[l, 1]
        for v in range(per):
            amps = rx_list([get(i, rows(v)) for i in range(BLOCKS)], c, s)
            for i, (re, im) in enumerate(amps):
                dst[k, i, 0, rows(v), :] = re
                dst[k, i, 1, rows(v), :] = im

    def chunk_pair(k0, k1, l):
        c, s = tabs[l, 0], tabs[l, 1]

        def body(i):
            for v in range(per):
                p0 = work[k0, i, 0, rows(v), :], work[k0, i, 1, rows(v), :]
                p1 = work[k1, i, 0, rows(v), :], work[k1, i, 1, rows(v), :]
                p0, p1 = rx_pair(p0, p1, c, s)
                work[k0, i, 0, rows(v), :] = p0[0]
                work[k0, i, 1, rows(v), :] = p0[1]
                work[k1, i, 0, rows(v), :] = p1[0]
                work[k1, i, 1, rows(v), :] = p1[1]

        loop(0, BLOCKS, body)

    def half_bits(base, l):
        step = 1
        while step < half:
            def pair(i, step=step):
                k0 = base + i // step * 2 * step + i % step
                chunk_pair(k0, k0 + step, l)

            loop(0, half // 2, pair)
            step *= 2

    def ship(k, p):
        def one(i):
            j, dev = peer(i)
            put(send.at[k, j], recv.at[p, k, me], send_sem.at[k], recv_sem.at[p, k], dev).start()

        loop(0, 15, one)
        pltpu.make_async_copy(send.at[k, me], recv.at[p, k, me], recv_sem.at[p, k]).start()

    def sent(k):
        part = send.at[k, pl.ds(0, BLOCKS - 1)]
        pltpu.make_async_copy(part, part, send_sem.at[k]).wait()

    def arrived(k, p):
        pltpu.make_async_copy(recv.at[p, k], recv.at[p, k], recv_sem.at[p, k]).wait()

    def first_phase(k):
        return lambda i, r: (trig[k, 0, i, r, :], -trig[k, 1, i, r, :])

    def next_phase(k):
        def get(i, r):
            re, im = work[k, i, 0, r, :], work[k, i, 1, r, :]
            co, si = trig[k, 0, i, r, :], trig[k, 1, i, r, :]
            return re * co + im * si, im * co - re * si

        return get

    def collect(l, p, with_angles):
        def one(k, with_inner):
            if with_angles:
                angles(l + 1, 1 - p, k)
            arrived(k, p)
            block_bits(l, k, lambda i, r: (recv[p, k, i, 0, r, :], recv[p, k, i, 1, r, :]), work)
            if with_inner:
                inner(work, k, l)

        loop(0, half, lambda k: one(k, True))
        half_bits(0, l)
        loop(half, n, lambda k: one(k, False))
        half_bits(half, l)

    def start(k, with_inner):
        angles(0, 0, k)
        block_bits(0, k, first_phase(k), send)
        if with_inner:
            inner(send, k, 0)
        ship(k, 0)

    loop(0, half, lambda k: start(k, False))
    loop(half, n, lambda k: start(k, True))

    def costs(k):
        pltpu.make_async_copy(cost.at[1, k], cost.at[1, k], crecv_sem.at[k]).wait()
        part = cost.at[0, k, pl.ds(0, BLOCKS - 1)]
        pltpu.make_async_copy(part, part, csend_sem.at[k]).wait()

    loop(0, n, costs)

    def layer(l):
        p = l % 2
        collect(l, p, True)

        def resend(k, late):
            if not late:
                chunk_pair(k, k + half, l)
            sent(k)
            block_bits(l + 1, k, next_phase(k), send)
            if late:
                inner(send, k, l + 1)
            ship(k, 1 - p)

        loop(0, half, lambda k: resend(k, False))
        loop(half, n, lambda k: resend(k, True))

    loop(0, layers - 1, layer)

    last = layers - 1
    collect(last, last % 2, False)

    def store(part, out, k):
        return pltpu.make_async_copy(work.at[k, :, part], out.at[:, k], store_sem.at[part, k])

    def finish(k, acc):
        chunk_pair(k, k + half, last)
        for kk in (k, k + half):
            store(0, re_out, kk).start()
            store(1, im_out, kk).start()

            def add(i, acc, kk=kk):
                for v in range(per):
                    re, im = work[kk, i, 0, rows(v), :], work[kk, i, 1, rows(v), :]
                    acc = acc + cost[0, kk, i, rows(v), :] * (re * re + im * im)
                return acc

            acc = lax.fori_loop(0, BLOCKS, add, acc)
        return acc

    en_send[...] = lax.fori_loop(0, half, finish, jnp.zeros((SUBLANES, LANES), jnp.float32))
    loop(0, 15, lambda i: put(en_send, en_recv.at[me], esend_sem, erecv_sem, peer(i)[1]).start())
    pltpu.make_async_copy(en_send, en_recv.at[me], erecv_sem).start()

    def drain(k):
        sent(k)
        store(0, re_out, k).wait()
        store(1, im_out, k).wait()

    loop(0, n, drain)
    pltpu.make_async_copy(en_recv, en_recv, erecv_sem).wait()
    part = en_recv.at[pl.ds(0, BLOCKS - 1)]
    pltpu.make_async_copy(part, part, esend_sem).wait()
    full = en_recv[0]
    for i in range(1, BLOCKS):
        full = full + en_recv[i]
    en_out[0] = jnp.sum(full) / total


def solution(mesh):
    state_spec = P(("inst", "qx", "qy"))

    def device_body(cost_local, gammas, betas):
        local = cost_local.shape[0]
        vregs = local // (BLOCKS * SUBLANES * LANES)
        layers = gammas.shape[0]
        n = CHUNKS
        r = vregs // n * SUBLANES
        shape = (BLOCKS, n, r, LANES)
        f32 = jnp.float32
        any_spec = pl.BlockSpec(memory_space=pl.ANY)
        smem = pl.BlockSpec(memory_space=pltpu.SMEM)
        dma = pltpu.SemaphoreType.DMA
        energy, out_re, out_im = pl.pallas_call(
            functools.partial(kernel, layers, vregs, float(local * BLOCKS)),
            out_shape=[jax.ShapeDtypeStruct((1,), f32), jax.ShapeDtypeStruct(shape, f32),
                       jax.ShapeDtypeStruct(shape, f32)],
            in_specs=[any_spec, smem, smem],
            out_specs=[smem, any_spec, any_spec],
            scratch_shapes=[
                pltpu.VMEM((2, n, BLOCKS, r, LANES), f32),
                pltpu.VMEM((n, 2, BLOCKS, r, LANES), f32),
                pltpu.VMEM((2, n, BLOCKS, 2, r, LANES), f32),
                pltpu.VMEM((n, BLOCKS, 2, r, LANES), f32),
                pltpu.VMEM((n, BLOCKS, 2, r, LANES), f32),
                pltpu.VMEM((layers, 2, SUBLANES, LANES), f32),
                pltpu.VMEM((SUBLANES, LANES), f32),
                pltpu.VMEM((BLOCKS, SUBLANES, LANES), f32),
                dma((n,)), dma((n,)), dma((n,)), dma((n,)), dma((2, n)), dma, dma, dma((2, n)),
            ],
            compiler_params=pltpu.CompilerParams(collective_id=0, has_side_effects=True),
            name="qaoa",
        )(cost_local.reshape(shape), gammas, betas)
        return energy, out_re.reshape(local), out_im.reshape(local)

    return jax.shard_map(device_body, mesh=mesh, in_specs=(state_spec, P(), P()),
                         out_specs=(P("inst"), state_spec, state_spec), check_vma=False)
```

```python
import functools

import jax
import jax.numpy as jnp
from jax import lax
from jax.experimental import pallas as pl
from jax.experimental.pallas import tpu as pltpu
from jax.sharding import PartitionSpec as P

LANES = 128
SUBLANES = 8
BLOCKS = 16
CHUNKS = 8
GROUP = 4


def flip(x, m):
    return (x // 2 + m // 2) % 2 * 2 + (x + m) % 2


def rx_pair(a, b, c, s):
    (ar, ai), (br, bi) = a, b
    return (c * ar + s * bi, c * ai - s * br), (c * br + s * ai, c * bi - s * ar)


def rx_list(amps, c, s):
    amps = list(amps)
    step = 1
    while step < len(amps):
        for i in range(len(amps)):
            if not i & step:
                amps[i], amps[i + step] = rx_pair(amps[i], amps[i + step], c, s)
        step *= 2
    return amps


def kernel(layers, vregs, total, cost_in, gam, bet, en_out, re_out, im_out,
           cost, trig, recv, work, send, mats, tabs, en_send, en_recv,
           load_sem, csend_sem, crecv_sem, send_sem, recv_sem, esend_sem, erecv_sem, store_sem):
    n = CHUNKS
    half = n // 2
    per = vregs // n
    a, b = lax.axis_index("qx"), lax.axis_index("qy")
    me = a * 4 + b

    def loop(lo, hi, body):
        def step(i, carry):
            body(i)
            return carry

        lax.fori_loop(lo, hi, step, 0)

    def peer(i):
        m = 15 - i
        pa, pb = flip(a, m % 4), flip(b, m // 4)
        return pa * 4 + pb, {"qx": pa, "qy": pb}

    def put(src, dst, send_s, recv_s, dev):
        return pltpu.make_async_remote_copy(src, dst, send_s, recv_s, device_id=dev,
                                            device_id_type=pl.DeviceIdType.MESH)

    def load(k):
        return pltpu.make_async_copy(cost_in.at[:, k], cost.at[0, k], load_sem.at[k])

    loop(0, n, lambda k: load(k).start())
    barrier = pltpu.get_barrier_semaphore()
    loop(0, 15, lambda i: pl.semaphore_signal(barrier, inc=1, device_id=peer(i)[1],
                                              device_id_type=pl.DeviceIdType.MESH))
    pl.semaphore_wait(barrier, 15)

    def share(k):
        load(k).wait()

        def one(i):
            j, dev = peer(i)
            put(cost.at[0, k, j], cost.at[1, k, me], csend_sem.at[k], crecv_sem.at[k], dev).start()

        loop(0, 15, one)
        pltpu.make_async_copy(cost.at[0, k, me], cost.at[1, k, me], crecv_sem.at[k]).start()

    loop(0, n, share)

    def tables(l):
        angle = jnp.full((SUBLANES, LANES), 0.5 * bet[l], jnp.float32)
        tabs[l, 0] = jnp.cos(angle)
        tabs[l, 1] = jnp.sin(angle)
        c, s = tabs[l, 0][0:1, :], tabs[l, 1][0:1, :]
        row = lax.broadcasted_iota(jnp.int32, (LANES, LANES), 0)
        col = lax.broadcasted_iota(jnp.int32, (LANES, LANES), 1)
        size = jnp.ones((LANES, LANES), jnp.float32)
        count = jnp.zeros((LANES, LANES), jnp.int32)
        for q in range(7):
            differ = (row & (1 << q)) != (col & (1 << q))
            size = size * jnp.where(differ, s, c)
            count = count + jnp.where(differ, 1, 0)
        turn = count & 3
        m_re = jnp.where(turn == 0, size, jnp.where(turn == 2, -size, 0.0))
        m_im = jnp.where(turn == 3, size, jnp.where(turn == 1, -size, 0.0))
        mats[l, :LANES, :LANES] = m_re
        mats[l, :LANES, LANES:] = m_im
        mats[l, LANES:, :LANES] = -m_im
        mats[l, LANES:, LANES:] = m_re

    loop(0, layers, tables)

    def rows(v):
        return pl.ds(v * SUBLANES, SUBLANES)

    def angles(l, lay, k):
        g = gam[l]

        def body(i):
            for v in range(per):
                t = g * cost[lay, k, i, rows(v), :]
                trig[k, 0, i, rows(v), :] = jnp.cos(t)
                trig[k, 1, i, rows(v), :] = jnp.sin(t)

        loop(0, BLOCKS, body)

    def inner(buf, k, l):
        size = BLOCKS * per * SUBLANES
        x = jnp.concatenate([buf[k, :, 0].reshape(size, LANES), buf[k, :, 1].reshape(size, LANES)], axis=1)
        y = jnp.dot(x, mats[l], precision=lax.Precision.HIGHEST, preferred_element_type=jnp.float32)
        buf[k, :, 0] = y[:, :LANES].reshape(BLOCKS, per * SUBLANES, LANES)
        buf[k, :, 1] = y[:, LANES:].reshape(BLOCKS, per * SUBLANES, LANES)
        c, s = tabs[l, 0], tabs[l, 1]
        place = lax.broadcasted_iota(jnp.int32, (SUBLANES, LANES), 0)

        def partner(v, step):
            if 2 * step == SUBLANES:
                return pltpu.roll(v, step, 0)
            return jnp.where((place & step) != 0, pltpu.roll(v, step, 0), pltpu.roll(v, SUBLANES - step, 0))

        def body(g):
            for i in range(GROUP):
                i = g * GROUP + i
                amps = []
                for v in range(per):
                    re, im = buf[k, i, 0, rows(v), :], buf[k, i, 1, rows(v), :]
                    for step in (1, 2, 4):
                        pr, pi = partner(re, step), partner(im, step)
                        re, im = c * re + s * pi, c * im - s * pr
                    amps.append((re, im))
                for v, (re, im) in enumerate(rx_list(amps, c, s)):
                    buf[k, i, 0, rows(v), :] = re
                    buf[k, i, 1, rows(v), :] = im

        loop(0, BLOCKS // GROUP, body)

    def block_bits(l, k, get, dst):
        c, s = tabs[l, 0], tabs[l, 1]
        for v in range(per):
            amps = rx_list([get(i, rows(v)) for i in range(BLOCKS)], c, s)
            for i, (re, im) in enumerate(amps):
                dst[k, i, 0, rows(v), :] = re
                dst[k, i, 1, rows(v), :] = im

    def chunk_pair(k0, k1, l):
        c, s = tabs[l, 0], tabs[l, 1]

        def body(i):
            for v in range(per):
                p0 = work[k0, i, 0, rows(v), :], work[k0, i, 1, rows(v), :]
                p1 = work[k1, i, 0, rows(v), :], work[k1, i, 1, rows(v), :]
                p0, p1 = rx_pair(p0, p1, c, s)
                work[k0, i, 0, rows(v), :] = p0[0]
                work[k0, i, 1, rows(v), :] = p0[1]
                work[k1, i, 0, rows(v), :] = p1[0]
                work[k1, i, 1, rows(v), :] = p1[1]

        loop(0, BLOCKS, body)

    def half_bits(base, l):
        step = 1
        while step < half:
            def pair(i, step=step):
                k0 = base + i // step * 2 * step + i % step
                chunk_pair(k0, k0 + step, l)

            loop(0, half // 2, pair)
            step *= 2

    def ship(k, p):
        def one(i):
            j, dev = peer(i)
            put(send.at[k, j], recv.at[p, k, me], send_sem.at[k], recv_sem.at[p, k], dev).start()

        loop(0, 15, one)
        pltpu.make_async_copy(send.at[k, me], recv.at[p, k, me], recv_sem.at[p, k]).start()

    def sent(k):
        part = send.at[k, pl.ds(0, BLOCKS - 1)]
        pltpu.make_async_copy(part, part, send_sem.at[k]).wait()

    def arrived(k, p):
        pltpu.make_async_copy(recv.at[p, k], recv.at[p, k], recv_sem.at[p, k]).wait()

    def first_phase(k):
        return lambda i, r: (trig[k, 0, i, r, :], -trig[k, 1, i, r, :])

    def next_phase(k):
        def get(i, r):
            re, im = work[k, i, 0, r, :], work[k, i, 1, r, :]
            co, si = trig[k, 0, i, r, :], trig[k, 1, i, r, :]
            return re * co + im * si, im * co - re * si

        return get

    def collect(l, p, with_angles):
        def one(k, with_inner):
            if with_angles:
                angles(l + 1, 1 - p, k)
            arrived(k, p)
            block_bits(l, k, lambda i, r: (recv[p, k, i, 0, r, :], recv[p, k, i, 1, r, :]), work)
            if with_inner:
                inner(work, k, l)

        loop(0, half, lambda k: one(k, True))
        half_bits(0, l)
        loop(half, n, lambda k: one(k, False))
        half_bits(half, l)

    def start(k, with_inner):
        angles(0, 0, k)
        block_bits(0, k, first_phase(k), send)
        if with_inner:
            inner(send, k, 0)
        ship(k, 0)

    loop(0, half, lambda k: start(k, False))
    loop(half, n, lambda k: start(k, True))

    def costs(k):
        pltpu.make_async_copy(cost.at[1, k], cost.at[1, k], crecv_sem.at[k]).wait()
        part = cost.at[0, k, pl.ds(0, BLOCKS - 1)]
        pltpu.make_async_copy(part, part, csend_sem.at[k]).wait()

    loop(0, n, costs)

    def layer(l):
        p = l % 2
        collect(l, p, True)

        def resend(k, late):
            if not late:
                chunk_pair(k, k + half, l)
            sent(k)
            block_bits(l + 1, k, next_phase(k), send)
            if late:
                inner(send, k, l + 1)
            ship(k, 1 - p)

        loop(0, half, lambda k: resend(k, False))
        loop(half, n, lambda k: resend(k, True))

    loop(0, layers - 1, layer)

    last = layers - 1
    collect(last, last % 2, False)

    def store(part, out, k):
        return pltpu.make_async_copy(work.at[k, :, part], out.at[:, k], store_sem.at[part, k])

    def finish(k, acc):
        chunk_pair(k, k + half, last)
        for kk in (k, k + half):
            store(0, re_out, kk).start()
            store(1, im_out, kk).start()

            def add(i, acc, kk=kk):
                for v in range(per):
                    re, im = work[kk, i, 0, rows(v), :], work[kk, i, 1, rows(v), :]
                    acc = acc + cost[0, kk, i, rows(v), :] * (re * re + im * im)
                return acc

            acc = lax.fori_loop(0, BLOCKS, add, acc)
        return acc

    en_send[...] = lax.fori_loop(0, half, finish, jnp.zeros((SUBLANES, LANES), jnp.float32))
    loop(0, 15, lambda i: put(en_send, en_recv.at[me], esend_sem, erecv_sem, peer(i)[1]).start())
    pltpu.make_async_copy(en_send, en_recv.at[me], erecv_sem).start()

    def drain(k):
        sent(k)
        store(0, re_out, k).wait()
        store(1, im_out, k).wait()

    loop(0, n, drain)
    pltpu.make_async_copy(en_recv, en_recv, erecv_sem).wait()
    part = en_recv.at[pl.ds(0, BLOCKS - 1)]
    pltpu.make_async_copy(part, part, esend_sem).wait()
    full = en_recv[0]
    for i in range(1, BLOCKS):
        full = full + en_recv[i]
    en_out[0] = jnp.sum(full) / total


def solution(mesh):
    state_spec = P(("inst", "qx", "qy"))

    def device_body(cost_local, gammas, betas):
        local = cost_local.shape[0]
        vregs = local // (BLOCKS * SUBLANES * LANES)
        layers = gammas.shape[0]
        n = CHUNKS
        r = vregs // n * SUBLANES
        shape = (BLOCKS, n, r, LANES)
        f32 = jnp.float32
        any_spec = pl.BlockSpec(memory_space=pl.ANY)
        smem = pl.BlockSpec(memory_space=pltpu.SMEM)
        dma = pltpu.SemaphoreType.DMA
        energy, out_re, out_im = pl.pallas_call(
            functools.partial(kernel, layers, vregs, float(local * BLOCKS)),
            out_shape=[jax.ShapeDtypeStruct((1,), f32), jax.ShapeDtypeStruct(shape, f32),
                       jax.ShapeDtypeStruct(shape, f32)],
            in_specs=[any_spec, smem, smem],
            out_specs=[smem, any_spec, any_spec],
            scratch_shapes=[
                pltpu.VMEM((2, n, BLOCKS, r, LANES), f32),
                pltpu.VMEM((n, 2, BLOCKS, r, LANES), f32),
                pltpu.VMEM((2, n, BLOCKS, 2, r, LANES), f32),
                pltpu.VMEM((n, BLOCKS, 2, r, LANES), f32),
                pltpu.VMEM((n, BLOCKS, 2, r, LANES), f32),
                pltpu.VMEM((layers, 2 * LANES, 2 * LANES), f32),
                pltpu.VMEM((layers, 2, SUBLANES, LANES), f32),
                pltpu.VMEM((SUBLANES, LANES), f32),
                pltpu.VMEM((BLOCKS, SUBLANES, LANES), f32),
                dma((n,)), dma((n,)), dma((n,)), dma((n,)), dma((2, n)), dma, dma, dma((2, n)),
            ],
            compiler_params=pltpu.CompilerParams(collective_id=0, has_side_effects=True),
            name="qaoa",
        )(cost_local.reshape(shape), gammas, betas)
        return energy, out_re.reshape(local), out_im.reshape(local)

    return jax.shard_map(device_body, mesh=mesh, in_specs=(state_spec, P(), P()),
                         out_specs=(P("inst"), state_spec, state_spec), check_vma=False)
```

```python
import functools

import jax
import jax.numpy as jnp
from jax import lax
from jax.experimental import pallas as pl
from jax.experimental.pallas import tpu as pltpu
from jax.sharding import PartitionSpec as P

LANES = 128
SUBLANES = 8
BLOCKS = 16
CHUNKS = 8
GROUPS = ((0, 1), (1, 3), (4, 3), (7, 1))
GROUP = 4


def flip(x, m):
    return (x // 2 + m // 2) % 2 * 2 + (x + m) % 2


def rx_pair(a, b, c, s):
    (ar, ai), (br, bi) = a, b
    return (c * ar + s * bi, c * ai - s * br), (c * br + s * ai, c * bi - s * ar)


def rx_list(amps, c, s):
    amps = list(amps)
    step = 1
    while step < len(amps):
        for i in range(len(amps)):
            if not i & step:
                amps[i], amps[i + step] = rx_pair(amps[i], amps[i + step], c, s)
        step *= 2
    return amps


def kernel(layers, vregs, total, cost_in, gam, bet, en_out, work,
           cost, trig, recv, send, mats, tabs, en_send, en_recv,
           load_sem, csend_sem, crecv_sem, send_sem, recv_sem, esend_sem, erecv_sem):
    n = CHUNKS
    half = n // 2
    per = vregs // n
    a, b = lax.axis_index("qx"), lax.axis_index("qy")
    me = a * 4 + b

    def loop(lo, hi, body):
        def step(i, carry):
            body(i)
            return carry

        lax.fori_loop(lo, hi, step, 0)

    def peer(i):
        m = 15 - i
        pa, pb = flip(a, m % 4), flip(b, m // 4)
        return pa * 4 + pb, {"qx": pa, "qy": pb}

    def put(src, dst, send_s, recv_s, dev):
        return pltpu.make_async_remote_copy(src, dst, send_s, recv_s, device_id=dev,
                                            device_id_type=pl.DeviceIdType.MESH)

    load = pltpu.make_async_copy(cost_in, cost.at[0], load_sem)
    load.start()
    barrier = pltpu.get_barrier_semaphore()
    loop(0, 15, lambda i: pl.semaphore_signal(barrier, inc=1, device_id=peer(i)[1],
                                              device_id_type=pl.DeviceIdType.MESH))
    pl.semaphore_wait(barrier, 15)
    load.wait()

    def share(i):
        j, dev = peer(i)
        put(cost.at[0, j], cost.at[1, me], csend_sem, crecv_sem, dev).start()

    loop(0, 15, share)
    pltpu.make_async_copy(cost.at[0, me], cost.at[1, me], crecv_sem).start()

    def tables(l):
        angle = jnp.full((SUBLANES, LANES), 0.5 * bet[l], jnp.float32)
        tabs[l, 0] = jnp.cos(angle)
        tabs[l, 1] = jnp.sin(angle)
        c, s = tabs[l, 0][0:1, :], tabs[l, 1][0:1, :]
        row = lax.broadcasted_iota(jnp.int32, (LANES, LANES), 0)
        col = lax.broadcasted_iota(jnp.int32, (LANES, LANES), 1)
        size = jnp.ones((LANES, LANES), jnp.float32)
        count = jnp.zeros((LANES, LANES), jnp.int32)
        for q in range(7):
            differ = (row & (1 << q)) != (col & (1 << q))
            size = size * jnp.where(differ, s, c)
            count = count + jnp.where(differ, 1, 0)
        turn = count & 3
        m_re = jnp.where(turn == 0, size, jnp.where(turn == 2, -size, 0.0))
        m_im = jnp.where(turn == 3, size, jnp.where(turn == 1, -size, 0.0))
        mats[l, :LANES, :LANES] = m_re
        mats[l, :LANES, LANES:] = m_im
        mats[l, LANES:, :LANES] = -m_im
        mats[l, LANES:, LANES:] = m_re

    loop(0, layers, tables)

    def rows(v):
        return pl.ds(v * SUBLANES, SUBLANES)

    def take(buf, k, i, r):
        return buf[i, k, 0, r, :], buf[i, k, 1, r, :]

    def keep(buf, k, i, r, amp):
        buf[i, k, 0, r, :] = amp[0]
        buf[i, k, 1, r, :] = amp[1]

    def angles(l, lay, k):
        g = gam[l]

        def body(i):
            for v in range(per):
                t = g * cost[lay, i, k, rows(v), :]
                keep(trig, k, i, rows(v), (jnp.cos(t), jnp.sin(t)))

        loop(0, BLOCKS, body)

    def inner(buf, k, l):
        size = BLOCKS * per * SUBLANES
        x = jnp.concatenate([buf[:, k, 0].reshape(size, LANES), buf[:, k, 1].reshape(size, LANES)], axis=1)
        y = jnp.dot(x, mats[l], precision=lax.Precision.HIGHEST, preferred_element_type=jnp.float32)
        buf[:, k, 0] = y[:, :LANES].reshape(BLOCKS, per * SUBLANES, LANES)
        buf[:, k, 1] = y[:, LANES:].reshape(BLOCKS, per * SUBLANES, LANES)
        c, s = tabs[l, 0], tabs[l, 1]
        place = lax.broadcasted_iota(jnp.int32, (SUBLANES, LANES), 0)

        def partner(v, step):
            if 2 * step == SUBLANES:
                return pltpu.roll(v, step, 0)
            return jnp.where((place & step) != 0, pltpu.roll(v, step, 0), pltpu.roll(v, SUBLANES - step, 0))

        def body(g):
            for i in range(GROUP):
                i = g * GROUP + i
                amps = []
                for v in range(per):
                    re, im = take(buf, k, i, rows(v))
                    for step in (1, 2, 4):
                        pr, pi = partner(re, step), partner(im, step)
                        re, im = c * re + s * pi, c * im - s * pr
                    amps.append((re, im))
                for v, amp in enumerate(rx_list(amps, c, s)):
                    keep(buf, k, i, rows(v), amp)

        loop(0, BLOCKS // GROUP, body)

    def block_bits(l, k, get, dst):
        c, s = tabs[l, 0], tabs[l, 1]
        for v in range(per):
            amps = rx_list([get(i, rows(v)) for i in range(BLOCKS)], c, s)
            for i, amp in enumerate(amps):
                keep(dst, k, i, rows(v), amp)

    def chunk_pair(k0, k1, l):
        c, s = tabs[l, 0], tabs[l, 1]

        def body(i):
            for v in range(per):
                p0, p1 = rx_pair(take(work, k0, i, rows(v)), take(work, k1, i, rows(v)), c, s)
                keep(work, k0, i, rows(v), p0)
                keep(work, k1, i, rows(v), p1)

        loop(0, BLOCKS, body)

    def ship(group, p):
        lo, size = group
        part = pl.ds(lo, size)
        at = GROUPS.index(group)

        def one(i):
            j, dev = peer(i)
            put(send.at[j, part], recv.at[p, me, part], send_sem.at[at], recv_sem.at[p, at], dev).start()

        loop(0, 15, one)
        pltpu.make_async_copy(send.at[me, part], recv.at[p, me, part], recv_sem.at[p, at]).start()

    def sent():
        for at, (lo, size) in enumerate(GROUPS):
            part = send.at[pl.ds(0, BLOCKS - 1), pl.ds(lo, size)]
            pltpu.make_async_copy(part, part, send_sem.at[at]).wait()

    def arrived(group, p):
        lo, size = group
        part = recv.at[p, :, pl.ds(lo, size)]
        pltpu.make_async_copy(part, part, recv_sem.at[p, GROUPS.index(group)]).wait()

    def phased(k, get):
        def phased_get(i, r):
            (re, im), (co, si) = get(i, r), take(trig, k, i, r)
            return re * co + im * si, im * co - re * si

        return phased_get

    def collect(l, p, with_angles):
        def fetch(k):
            block_bits(l, k, lambda i, r: take(recv.at[p], k, i, r), work)

        def early(k):
            fetch(k)
            inner(work, k, l)

        for group in GROUPS:
            lo, size = group
            hi = lo + size
            if with_angles and lo in (0, half):
                loop(lo, lo + half, lambda k: angles(l + 1, 1 - p, k))
            arrived(group, p)
            if hi <= half:
                loop(lo, hi, early)
            else:
                loop(lo, hi, fetch)
            if hi == half:
                loop(0, 2, lambda i: chunk_pair(2 * i, 2 * i + 1, l))
                loop(0, 2, lambda i: chunk_pair(i, i + 2, l))
            if hi == n - 1:
                chunk_pair(4, 5, l)

    def first_chunk(l):
        c, s = tabs[l, 0], tabs[l, 1]

        def get(i, r):
            upper = rx_pair(take(work, 6, i, r), take(work, 7, i, r), c, s)[0]
            upper = rx_pair(take(work, 4, i, r), upper, c, s)[0]
            return rx_pair(take(work, 0, i, r), upper, c, s)[0]

        return get

    def rest(l):
        chunk_pair(6, 7, l)
        loop(0, 2, lambda i: chunk_pair(4 + i, 6 + i, l))

    def start(k, late):
        angles(0, 0, k)
        block_bits(0, k, lambda i, r: (trig[i, k, 0, r, :], -trig[i, k, 1, r, :]), send)
        if late:
            inner(send, k, 0)

    for group in GROUPS:
        lo, size = group
        loop(lo, lo + size, lambda k: start(k, lo >= half))
        ship(group, 0)

    pltpu.make_async_copy(cost.at[1], cost.at[1], crecv_sem).wait()
    part = cost.at[0, pl.ds(0, BLOCKS - 1)]
    pltpu.make_async_copy(part, part, csend_sem).wait()

    def layer(l):
        p = l % 2
        collect(l, p, True)
        sent()
        for group in GROUPS:
            lo, size = group
            if lo == 0:
                block_bits(l + 1, 0, phased(0, first_chunk(l)), send)
                ship(group, 1 - p)
                rest(l)
                loop(0, half, lambda k: chunk_pair(k, k + half, l))
                continue

            def resend(k):
                block_bits(l + 1, k, phased(k, lambda i, r: take(work, k, i, r)), send)
                if lo >= half:
                    inner(send, k, l + 1)

            loop(lo, lo + size, resend)
            ship(group, 1 - p)

    loop(0, layers - 1, layer)

    last = layers - 1
    collect(last, last % 2, False)
    rest(last)
    c, s = tabs[last, 0], tabs[last, 1]

    def finish(k, acc):
        def body(i, acc):
            for v in range(per):
                r = rows(v)
                pair = rx_pair(take(work, k, i, r), take(work, k + half, i, r), c, s)
                for kk, (re, im) in zip((k, k + half), pair):
                    keep(work, kk, i, r, (re, im))
                    acc = acc + cost[0, i, kk, r, :] * (re * re + im * im)
            return acc

        return lax.fori_loop(0, BLOCKS, body, acc)

    en_send[...] = lax.fori_loop(0, half, finish, jnp.zeros((SUBLANES, LANES), jnp.float32))
    loop(0, 15, lambda i: put(en_send, en_recv.at[me], esend_sem, erecv_sem, peer(i)[1]).start())
    pltpu.make_async_copy(en_send, en_recv.at[me], erecv_sem).start()
    sent()
    pltpu.make_async_copy(en_recv, en_recv, erecv_sem).wait()
    part = en_recv.at[pl.ds(0, BLOCKS - 1)]
    pltpu.make_async_copy(part, part, esend_sem).wait()
    full = en_recv[0]
    for i in range(1, BLOCKS):
        full = full + en_recv[i]
    en_out[0] = jnp.sum(full) / total


def split_kernel(pair, re_out, im_out, sem):
    copies = [pltpu.make_async_copy(pair.at[:, :, part], out, sem.at[part])
              for part, out in enumerate((re_out, im_out))]
    for copy in copies:
        copy.start()
    for copy in copies:
        copy.wait()


def solution(mesh):
    state_spec = P(("inst", "qx", "qy"))

    def device_body(cost_local, gammas, betas):
        local = cost_local.shape[0]
        vregs = local // (BLOCKS * SUBLANES * LANES)
        layers = gammas.shape[0]
        n = CHUNKS
        r = vregs // n * SUBLANES
        shape = (BLOCKS, n, r, LANES)
        pair = (BLOCKS, n, 2, r, LANES)
        f32 = jnp.float32
        any_spec = pl.BlockSpec(memory_space=pl.ANY)
        smem = pl.BlockSpec(memory_space=pltpu.SMEM)
        vmem = pl.BlockSpec(memory_space=pltpu.VMEM)
        dma = pltpu.SemaphoreType.DMA
        g = len(GROUPS)
        energy, state = pl.pallas_call(
            functools.partial(kernel, layers, vregs, float(local * BLOCKS)),
            out_shape=[jax.ShapeDtypeStruct((1,), f32), pltpu.VMEM(pair, f32)],
            in_specs=[any_spec, smem, smem],
            out_specs=[smem, vmem],
            scratch_shapes=[
                pltpu.VMEM((2,) + shape, f32),
                pltpu.VMEM(pair, f32),
                pltpu.VMEM((2,) + pair, f32),
                pltpu.VMEM(pair, f32),
                pltpu.VMEM((layers, 2 * LANES, 2 * LANES), f32),
                pltpu.VMEM((layers, 2, SUBLANES, LANES), f32),
                pltpu.VMEM((SUBLANES, LANES), f32),
                pltpu.VMEM((BLOCKS, SUBLANES, LANES), f32),
                dma, dma, dma, dma((g,)), dma((2, g)), dma, dma,
            ],
            compiler_params=pltpu.CompilerParams(collective_id=0, has_side_effects=True),
            name="qaoa",
        )(cost_local.reshape(shape), gammas, betas)
        out_re, out_im = pl.pallas_call(
            split_kernel,
            out_shape=[jax.ShapeDtypeStruct(shape, f32)] * 2,
            in_specs=[vmem],
            out_specs=[any_spec] * 2,
            scratch_shapes=[dma((2,))],
            name="split",
        )(pltpu.with_memory_space_constraint(state, pltpu.VMEM))
        return energy, out_re.reshape(local), out_im.reshape(local)

    return jax.shard_map(device_body, mesh=mesh, in_specs=(state_spec, P(), P()),
                         out_specs=(P("inst"), state_spec, state_spec), check_vma=False)
```

```python
import functools

import jax
import jax.numpy as jnp
from jax import lax
from jax.experimental import pallas as pl
from jax.experimental.pallas import tpu as pltpu
from jax.sharding import PartitionSpec as P

LANES = 128
SUBLANES = 8
BLOCKS = 16
CHUNKS = 8
GROUPS = ((0, 1), (1, 3), (4, 3), (7, 1))
GROUP = 4


def flip(x, m):
    return (x // 2 + m // 2) % 2 * 2 + (x + m) % 2


def rx_pair(a, b, c, s):
    (ar, ai), (br, bi) = a, b
    return (c * ar + s * bi, c * ai - s * br), (c * br + s * ai, c * bi - s * ar)


def rx_list(amps, c, s):
    amps = list(amps)
    step = 1
    while step < len(amps):
        for i in range(len(amps)):
            if not i & step:
                amps[i], amps[i + step] = rx_pair(amps[i], amps[i + step], c, s)
        step *= 2
    return amps


def kernel(layers, vregs, total, cost_in, gam, bet, en_out, work,
           cost, trig, recv, send, mats, tabs, en_send, en_recv,
           load_sem, csend_sem, crecv_sem, send_sem, recv_sem, esend_sem, erecv_sem):
    n = CHUNKS
    half = n // 2
    per = vregs // n
    a, b = lax.axis_index("qx"), lax.axis_index("qy")
    me = a * 4 + b

    def loop(lo, hi, body):
        def step(i, carry):
            body(i)
            return carry

        lax.fori_loop(lo, hi, step, 0)

    def peer(i):
        m = 15 - i
        pa, pb = flip(a, m % 4), flip(b, m // 4)
        return pa * 4 + pb, {"qx": pa, "qy": pb}

    def put(src, dst, send_s, recv_s, dev):
        return pltpu.make_async_remote_copy(src, dst, send_s, recv_s, device_id=dev,
                                            device_id_type=pl.DeviceIdType.MESH)

    load = pltpu.make_async_copy(cost_in, cost.at[0], load_sem)
    load.start()
    barrier = pltpu.get_barrier_semaphore()
    loop(0, 15, lambda i: pl.semaphore_signal(barrier, inc=1, device_id=peer(i)[1],
                                              device_id_type=pl.DeviceIdType.MESH))
    pl.semaphore_wait(barrier, 15)
    load.wait()

    def share(i):
        j, dev = peer(i)
        put(cost.at[0, j], cost.at[1, me], csend_sem, crecv_sem, dev).start()

    loop(0, 15, share)
    cost[1, me] = cost[0, me]

    def tables(l):
        angle = jnp.full((SUBLANES, LANES), 0.5 * bet[l], jnp.float32)
        tabs[l, 0] = jnp.cos(angle)
        tabs[l, 1] = jnp.sin(angle)
        c, s = tabs[l, 0][0:1, :], tabs[l, 1][0:1, :]
        row = lax.broadcasted_iota(jnp.int32, (LANES, LANES), 0)
        col = lax.broadcasted_iota(jnp.int32, (LANES, LANES), 1)
        size = jnp.ones((LANES, LANES), jnp.float32)
        count = jnp.zeros((LANES, LANES), jnp.int32)
        for q in range(7):
            differ = (row & (1 << q)) != (col & (1 << q))
            size = size * jnp.where(differ, s, c)
            count = count + jnp.where(differ, 1, 0)
        turn = count & 3
        m_re = jnp.where(turn == 0, size, jnp.where(turn == 2, -size, 0.0))
        m_im = jnp.where(turn == 3, size, jnp.where(turn == 1, -size, 0.0))
        mats[l, :LANES, :LANES] = m_re
        mats[l, :LANES, LANES:] = m_im
        mats[l, LANES:, :LANES] = -m_im
        mats[l, LANES:, LANES:] = m_re

    loop(0, layers, tables)

    def rows(v):
        return pl.ds(v * SUBLANES, SUBLANES)

    def take(buf, k, i, r):
        return buf[i, k, 0, r, :], buf[i, k, 1, r, :]

    def keep(buf, k, i, r, amp):
        buf[i, k, 0, r, :] = amp[0]
        buf[i, k, 1, r, :] = amp[1]

    def angles(l, lay, k):
        g = gam[l]

        def body(i):
            for v in range(per):
                t = g * cost[lay, i, k, rows(v), :]
                keep(trig, k, i, rows(v), (jnp.cos(t), jnp.sin(t)))

        loop(0, BLOCKS, body)

    def inner(buf, k, l):
        size = BLOCKS * per * SUBLANES
        x = jnp.concatenate([buf[:, k, 0].reshape(size, LANES), buf[:, k, 1].reshape(size, LANES)], axis=1)
        y = jnp.dot(x, mats[l], precision=lax.Precision.HIGHEST, preferred_element_type=jnp.float32)
        buf[:, k, 0] = y[:, :LANES].reshape(BLOCKS, per * SUBLANES, LANES)
        buf[:, k, 1] = y[:, LANES:].reshape(BLOCKS, per * SUBLANES, LANES)
        c, s = tabs[l, 0], tabs[l, 1]
        place = lax.broadcasted_iota(jnp.int32, (SUBLANES, LANES), 0)

        def partner(v, step):
            if 2 * step == SUBLANES:
                return pltpu.roll(v, step, 0)
            return jnp.where((place & step) != 0, pltpu.roll(v, step, 0), pltpu.roll(v, SUBLANES - step, 0))

        def body(g):
            for i in range(GROUP):
                i = g * GROUP + i
                amps = []
                for v in range(per):
                    re, im = take(buf, k, i, rows(v))
                    for step in (1, 2, 4):
                        pr, pi = partner(re, step), partner(im, step)
                        re, im = c * re + s * pi, c * im - s * pr
                    amps.append((re, im))
                for v, amp in enumerate(rx_list(amps, c, s)):
                    keep(buf, k, i, rows(v), amp)

        loop(0, BLOCKS // GROUP, body)

    def block_bits(l, k, get, dst):
        c, s = tabs[l, 0], tabs[l, 1]
        for v in range(per):
            amps = rx_list([get(i, rows(v)) for i in range(BLOCKS)], c, s)
            for i, amp in enumerate(amps):
                keep(dst, k, i, rows(v), amp)

    def chunk_pair(k0, k1, l):
        c, s = tabs[l, 0], tabs[l, 1]

        def body(i):
            for v in range(per):
                p0, p1 = rx_pair(take(work, k0, i, rows(v)), take(work, k1, i, rows(v)), c, s)
                keep(work, k0, i, rows(v), p0)
                keep(work, k1, i, rows(v), p1)

        loop(0, BLOCKS, body)

    def ship(group, p):
        lo, size = group
        part = pl.ds(lo, size)
        at = GROUPS.index(group)

        def one(i):
            j, dev = peer(i)
            put(send.at[p, j, part], recv.at[p, me, part], send_sem.at[p, at], recv_sem.at[p, at], dev).start()

        loop(0, 15, one)
        recv[p, me, part] = send[p, me, part]

    def sent(p):
        for at, (lo, size) in enumerate(GROUPS):
            part = send.at[p, pl.ds(0, BLOCKS - 1), pl.ds(lo, size)]
            pltpu.make_async_copy(part, part, send_sem.at[p, at]).wait()

    def arrived(group, p):
        lo, size = group
        part = recv.at[p, pl.ds(0, BLOCKS - 1), pl.ds(lo, size)]
        pltpu.make_async_copy(part, part, recv_sem.at[p, GROUPS.index(group)]).wait()

    def phased(k, get):
        def phased_get(i, r):
            (re, im), (co, si) = get(i, r), take(trig, k, i, r)
            return re * co + im * si, im * co - re * si

        return phased_get

    def collect(l, p, with_angles):
        def fetch(k):
            block_bits(l, k, lambda i, r: take(recv.at[p], k, i, r), work)

        def early(k):
            fetch(k)
            inner(work, k, l)

        for group in GROUPS:
            lo, size = group
            hi = lo + size
            if with_angles and lo in (0, half):
                loop(lo, lo + half, lambda k: angles(l + 1, 1 - p, k))
            arrived(group, p)
            if hi <= half:
                loop(lo, hi, early)
            else:
                loop(lo, hi, fetch)
            if hi == half:
                loop(0, 2, lambda i: chunk_pair(2 * i, 2 * i + 1, l))
                loop(0, 2, lambda i: chunk_pair(i, i + 2, l))
            if hi == n - 1:
                chunk_pair(4, 5, l)

    def first_chunk(l):
        c, s = tabs[l, 0], tabs[l, 1]

        def get(i, r):
            upper = rx_pair(take(work, 6, i, r), take(work, 7, i, r), c, s)[0]
            upper = rx_pair(take(work, 4, i, r), upper, c, s)[0]
            return rx_pair(take(work, 0, i, r), upper, c, s)[0]

        return get

    def rest(l):
        chunk_pair(6, 7, l)
        loop(0, 2, lambda i: chunk_pair(4 + i, 6 + i, l))

    def start(k, late):
        angles(0, 0, k)
        block_bits(0, k, lambda i, r: (trig[i, k, 0, r, :], -trig[i, k, 1, r, :]), send.at[0])
        if late:
            inner(send.at[0], k, 0)

    for group in GROUPS:
        lo, size = group
        loop(lo, lo + size, lambda k: start(k, lo >= half))
        ship(group, 0)

    part = cost.at[0, pl.ds(0, BLOCKS - 1)]
    pltpu.make_async_copy(part, part, crecv_sem).wait()
    pltpu.make_async_copy(part, part, csend_sem).wait()

    def layer(l):
        p = l % 2
        pl.when(l > 0)(lambda: sent(1 - p))
        collect(l, p, True)
        for group in GROUPS:
            lo, size = group
            if lo == 0:
                block_bits(l + 1, 0, phased(0, first_chunk(l)), send.at[1 - p])
                ship(group, 1 - p)
                rest(l)
                loop(0, half, lambda k: chunk_pair(k, k + half, l))
                continue

            def resend(k):
                block_bits(l + 1, k, phased(k, lambda i, r: take(work, k, i, r)), send.at[1 - p])
                if lo >= half:
                    inner(send.at[1 - p], k, l + 1)

            loop(lo, lo + size, resend)
            ship(group, 1 - p)

    loop(0, layers - 1, layer)

    last = layers - 1
    collect(last, last % 2, False)
    rest(last)
    c, s = tabs[last, 0], tabs[last, 1]

    def finish(k, acc):
        def body(i, acc):
            for v in range(per):
                r = rows(v)
                pair = rx_pair(take(work, k, i, r), take(work, k + half, i, r), c, s)
                for kk, (re, im) in zip((k, k + half), pair):
                    keep(work, kk, i, r, (re, im))
                    acc = acc + cost[0, i, kk, r, :] * (re * re + im * im)
            return acc

        return lax.fori_loop(0, BLOCKS, body, acc)

    en_send[...] = lax.fori_loop(0, half, finish, jnp.zeros((SUBLANES, LANES), jnp.float32))
    loop(0, 15, lambda i: put(en_send, en_recv.at[me], esend_sem, erecv_sem, peer(i)[1]).start())
    en_recv[me] = en_send[...]
    part = en_recv.at[pl.ds(0, BLOCKS - 1)]
    sent(1 - last % 2)
    sent(last % 2)
    pltpu.make_async_copy(part, part, erecv_sem).wait()
    pltpu.make_async_copy(part, part, esend_sem).wait()
    full = en_recv[0]
    for i in range(1, BLOCKS):
        full = full + en_recv[i]
    en_out[0] = jnp.sum(full) / total


def split_kernel(pair, re_out, im_out, sem):
    copies = [pltpu.make_async_copy(pair.at[:, :, part], out, sem.at[part])
              for part, out in enumerate((re_out, im_out))]
    for copy in copies:
        copy.start()
    for copy in copies:
        copy.wait()


def solution(mesh):
    state_spec = P(("inst", "qx", "qy"))

    def device_body(cost_local, gammas, betas):
        local = cost_local.shape[0]
        vregs = local // (BLOCKS * SUBLANES * LANES)
        layers = gammas.shape[0]
        n = CHUNKS
        r = vregs // n * SUBLANES
        shape = (BLOCKS, n, r, LANES)
        pair = (BLOCKS, n, 2, r, LANES)
        f32 = jnp.float32
        any_spec = pl.BlockSpec(memory_space=pl.ANY)
        smem = pl.BlockSpec(memory_space=pltpu.SMEM)
        vmem = pl.BlockSpec(memory_space=pltpu.VMEM)
        dma = pltpu.SemaphoreType.DMA
        g = len(GROUPS)
        energy, state = pl.pallas_call(
            functools.partial(kernel, layers, vregs, float(local * BLOCKS)),
            out_shape=[jax.ShapeDtypeStruct((1,), f32), pltpu.VMEM(pair, f32)],
            in_specs=[any_spec, smem, smem],
            out_specs=[smem, vmem],
            scratch_shapes=[
                pltpu.VMEM((2,) + shape, f32),
                pltpu.VMEM(pair, f32),
                pltpu.VMEM((2,) + pair, f32),
                pltpu.VMEM((2,) + pair, f32),
                pltpu.VMEM((layers, 2 * LANES, 2 * LANES), f32),
                pltpu.VMEM((layers, 2, SUBLANES, LANES), f32),
                pltpu.VMEM((SUBLANES, LANES), f32),
                pltpu.VMEM((BLOCKS, SUBLANES, LANES), f32),
                dma, dma, dma, dma((2, g)), dma((2, g)), dma, dma,
            ],
            compiler_params=pltpu.CompilerParams(collective_id=0, has_side_effects=True),
            name="qaoa",
        )(cost_local.reshape(shape), gammas, betas)
        out_re, out_im = pl.pallas_call(
            split_kernel,
            out_shape=[jax.ShapeDtypeStruct(shape, f32)] * 2,
            in_specs=[vmem],
            out_specs=[any_spec] * 2,
            scratch_shapes=[dma((2,))],
            name="split",
        )(pltpu.with_memory_space_constraint(state, pltpu.VMEM))
        return energy, out_re.reshape(local), out_im.reshape(local)

    return jax.shard_map(device_body, mesh=mesh, in_specs=(state_spec, P(), P()),
                         out_specs=(P("inst"), state_spec, state_spec), check_vma=False)
```

```python
import functools

import jax
import jax.numpy as jnp
from jax import lax
from jax.experimental import pallas as pl
from jax.experimental.pallas import tpu as pltpu
from jax.sharding import PartitionSpec as P

LANES = 128
SUBLANES = 8
BLOCKS = 16
CHUNKS = 8
GROUPS = ((0, 2), (2, 2), (4, 2), (6, 2))
GROUP = 4


def flip(x, m):
    return (x // 2 + m // 2) % 2 * 2 + (x + m) % 2


def rx_pair(a, b, c, s):
    (ar, ai), (br, bi) = a, b
    return (c * ar + s * bi, c * ai - s * br), (c * br + s * ai, c * bi - s * ar)


def rx_list(amps, c, s):
    amps = list(amps)
    step = 1
    while step < len(amps):
        for i in range(len(amps)):
            if not i & step:
                amps[i], amps[i + step] = rx_pair(amps[i], amps[i + step], c, s)
        step *= 2
    return amps


def kernel(layers, vregs, total, cost_in, gam, bet, en_out, work,
           cost, trig, recv, send, mats, tabs, en_send, en_recv,
           load_sem, csend_sem, crecv_sem, send_sem, recv_sem, esend_sem, erecv_sem):
    n = CHUNKS
    half = n // 2
    per = vregs // n
    a, b = lax.axis_index("qx"), lax.axis_index("qy")
    me = a * 4 + b

    def loop(lo, hi, body):
        def step(i, carry):
            body(i)
            return carry

        lax.fori_loop(lo, hi, step, 0)

    def peer(i):
        m = 15 - i
        pa, pb = flip(a, m % 4), flip(b, m // 4)
        return pa * 4 + pb, {"qx": pa, "qy": pb}

    def put(src, dst, send_s, recv_s, dev):
        return pltpu.make_async_remote_copy(src, dst, send_s, recv_s, device_id=dev,
                                            device_id_type=pl.DeviceIdType.MESH)

    load = pltpu.make_async_copy(cost_in, cost.at[0], load_sem)
    load.start()
    barrier = pltpu.get_barrier_semaphore()
    loop(0, 15, lambda i: pl.semaphore_signal(barrier, inc=1, device_id=peer(i)[1],
                                              device_id_type=pl.DeviceIdType.MESH))
    pl.semaphore_wait(barrier, 15)
    load.wait()

    def share(i):
        j, dev = peer(i)
        put(cost.at[0, j], cost.at[1, me], csend_sem, crecv_sem, dev).start()

    loop(0, 15, share)
    cost[1, me] = cost[0, me]

    def tables(l):
        angle = jnp.full((SUBLANES, LANES), 0.5 * bet[l], jnp.float32)
        tabs[l, 0] = jnp.cos(angle)
        tabs[l, 1] = jnp.sin(angle)
        c, s = tabs[l, 0][0:1, :], tabs[l, 1][0:1, :]
        row = lax.broadcasted_iota(jnp.int32, (LANES, LANES), 0)
        col = lax.broadcasted_iota(jnp.int32, (LANES, LANES), 1)
        size = jnp.ones((LANES, LANES), jnp.float32)
        count = jnp.zeros((LANES, LANES), jnp.int32)
        for q in range(7):
            differ = (row & (1 << q)) != (col & (1 << q))
            size = size * jnp.where(differ, s, c)
            count = count + jnp.where(differ, 1, 0)
        turn = count & 3
        m_re = jnp.where(turn == 0, size, jnp.where(turn == 2, -size, 0.0))
        m_im = jnp.where(turn == 3, size, jnp.where(turn == 1, -size, 0.0))
        mats[l, :LANES, :LANES] = m_re
        mats[l, :LANES, LANES:] = m_im
        mats[l, LANES:, :LANES] = -m_im
        mats[l, LANES:, LANES:] = m_re

    loop(0, layers, tables)

    def rows(v):
        return pl.ds(v * SUBLANES, SUBLANES)

    def take(buf, k, i, r):
        return buf[i, k, 0, r, :], buf[i, k, 1, r, :]

    def keep(buf, k, i, r, amp):
        buf[i, k, 0, r, :] = amp[0]
        buf[i, k, 1, r, :] = amp[1]

    def angles(l, lay, k):
        g = gam[l]

        def body(i):
            for v in range(per):
                t = g * cost[lay, i, k, rows(v), :]
                keep(trig, k, i, rows(v), (jnp.cos(t), jnp.sin(t)))

        loop(0, BLOCKS, body)

    def inner(buf, k, l):
        size = BLOCKS * per * SUBLANES
        x = jnp.concatenate([buf[:, k, 0].reshape(size, LANES), buf[:, k, 1].reshape(size, LANES)], axis=1)
        y = jnp.dot(x, mats[l], precision=lax.Precision.HIGHEST, preferred_element_type=jnp.float32)
        buf[:, k, 0] = y[:, :LANES].reshape(BLOCKS, per * SUBLANES, LANES)
        buf[:, k, 1] = y[:, LANES:].reshape(BLOCKS, per * SUBLANES, LANES)
        c, s = tabs[l, 0], tabs[l, 1]
        place = lax.broadcasted_iota(jnp.int32, (SUBLANES, LANES), 0)

        def partner(v, step):
            if 2 * step == SUBLANES:
                return pltpu.roll(v, step, 0)
            return jnp.where((place & step) != 0, pltpu.roll(v, step, 0), pltpu.roll(v, SUBLANES - step, 0))

        def body(g):
            for i in range(GROUP):
                i = g * GROUP + i
                amps = []
                for v in range(per):
                    re, im = take(buf, k, i, rows(v))
                    for step in (1, 2, 4):
                        pr, pi = partner(re, step), partner(im, step)
                        re, im = c * re + s * pi, c * im - s * pr
                    amps.append((re, im))
                for v, amp in enumerate(rx_list(amps, c, s)):
                    keep(buf, k, i, rows(v), amp)

        loop(0, BLOCKS // GROUP, body)

    def block_bits(l, k, get, dst):
        c, s = tabs[l, 0], tabs[l, 1]
        for v in range(per):
            amps = rx_list([get(i, rows(v)) for i in range(BLOCKS)], c, s)
            for i, amp in enumerate(amps):
                keep(dst, k, i, rows(v), amp)

    def chunk_pair(k0, k1, l):
        c, s = tabs[l, 0], tabs[l, 1]

        def body(i):
            for v in range(per):
                p0, p1 = rx_pair(take(work, k0, i, rows(v)), take(work, k1, i, rows(v)), c, s)
                keep(work, k0, i, rows(v), p0)
                keep(work, k1, i, rows(v), p1)

        loop(0, BLOCKS, body)

    def ship(group, p):
        lo, size = group
        part = pl.ds(lo, size)
        at = GROUPS.index(group)

        def one(i):
            j, dev = peer(i)
            put(send.at[p, j, part], recv.at[p, me, part], send_sem.at[p, at], recv_sem.at[p, at], dev).start()

        loop(0, 15, one)
        recv[p, me, part] = send[p, me, part]

    def sent(p):
        for at, (lo, size) in enumerate(GROUPS):
            part = send.at[p, pl.ds(0, BLOCKS - 1), pl.ds(lo, size)]
            pltpu.make_async_copy(part, part, send_sem.at[p, at]).wait()

    def arrived(group, p):
        lo, size = group
        part = recv.at[p, pl.ds(0, BLOCKS - 1), pl.ds(lo, size)]
        pltpu.make_async_copy(part, part, recv_sem.at[p, GROUPS.index(group)]).wait()

    def phased(k, get):
        def phased_get(i, r):
            (re, im), (co, si) = get(i, r), take(trig, k, i, r)
            return re * co + im * si, im * co - re * si

        return phased_get

    def collect(l, p, with_angles):
        def fetch(k):
            block_bits(l, k, lambda i, r: take(recv.at[p], k, i, r), work)

        def early(k):
            fetch(k)
            inner(work, k, l)

        for group in GROUPS:
            lo, size = group
            hi = lo + size
            if with_angles and lo in (0, half):
                loop(lo, lo + half, lambda k: angles(l + 1, 1 - p, k))
            arrived(group, p)
            loop(lo, hi, early if hi <= half else fetch)
            if hi < n:
                chunk_pair(lo, lo + 1, l)
            if hi == half:
                loop(0, 2, lambda i: chunk_pair(i, i + 2, l))

    def first_chunk(l, k):
        c, s = tabs[l, 0], tabs[l, 1]

        def get(i, r):
            upper = rx_pair(take(work, 6 + k, i, r), take(work, 7 - k, i, r), c, s)[0]
            upper = rx_pair(take(work, 4 + k, i, r), upper, c, s)[0]
            return rx_pair(take(work, k, i, r), upper, c, s)[0]

        return get

    def rest(l):
        chunk_pair(6, 7, l)
        loop(0, 2, lambda i: chunk_pair(4 + i, 6 + i, l))

    def start(k, late):
        angles(0, 0, k)
        block_bits(0, k, lambda i, r: (trig[i, k, 0, r, :], -trig[i, k, 1, r, :]), send.at[0])
        if late:
            inner(send.at[0], k, 0)

    for group in GROUPS:
        lo, size = group
        loop(lo, lo + size, lambda k: start(k, lo >= half))
        ship(group, 0)

    part = cost.at[0, pl.ds(0, BLOCKS - 1)]
    pltpu.make_async_copy(part, part, crecv_sem).wait()
    pltpu.make_async_copy(part, part, csend_sem).wait()

    def layer(l):
        p = l % 2
        pl.when(l > 0)(lambda: sent(1 - p))
        collect(l, p, True)
        for group in GROUPS:
            lo, size = group
            if lo == 0:
                loop(0, 2, lambda k: block_bits(l + 1, k, phased(k, first_chunk(l, k)), send.at[1 - p]))
                ship(group, 1 - p)
                rest(l)
                loop(0, half, lambda k: chunk_pair(k, k + half, l))
                continue

            def resend(k):
                block_bits(l + 1, k, phased(k, lambda i, r: take(work, k, i, r)), send.at[1 - p])
                if lo >= half:
                    inner(send.at[1 - p], k, l + 1)

            loop(lo, lo + size, resend)
            ship(group, 1 - p)

    loop(0, layers - 1, layer)

    last = layers - 1
    collect(last, last % 2, False)
    rest(last)
    c, s = tabs[last, 0], tabs[last, 1]

    def finish(k, acc):
        def body(i, acc):
            for v in range(per):
                r = rows(v)
                pair = rx_pair(take(work, k, i, r), take(work, k + half, i, r), c, s)
                for kk, (re, im) in zip((k, k + half), pair):
                    keep(work, kk, i, r, (re, im))
                    acc = acc + cost[0, i, kk, r, :] * (re * re + im * im)
            return acc

        return lax.fori_loop(0, BLOCKS, body, acc)

    en_send[...] = lax.fori_loop(0, half, finish, jnp.zeros((SUBLANES, LANES), jnp.float32))
    loop(0, 15, lambda i: put(en_send, en_recv.at[me], esend_sem, erecv_sem, peer(i)[1]).start())
    en_recv[me] = en_send[...]
    part = en_recv.at[pl.ds(0, BLOCKS - 1)]
    sent(1 - last % 2)
    sent(last % 2)
    pltpu.make_async_copy(part, part, erecv_sem).wait()
    pltpu.make_async_copy(part, part, esend_sem).wait()
    full = en_recv[0]
    for i in range(1, BLOCKS):
        full = full + en_recv[i]
    en_out[0] = jnp.sum(full) / total


def split_kernel(pair, re_out, im_out, sem):
    copies = [pltpu.make_async_copy(pair.at[:, :, part], out, sem.at[part])
              for part, out in enumerate((re_out, im_out))]
    for copy in copies:
        copy.start()
    for copy in copies:
        copy.wait()


def solution(mesh):
    state_spec = P(("inst", "qx", "qy"))

    def device_body(cost_local, gammas, betas):
        local = cost_local.shape[0]
        vregs = local // (BLOCKS * SUBLANES * LANES)
        layers = gammas.shape[0]
        n = CHUNKS
        r = vregs // n * SUBLANES
        shape = (BLOCKS, n, r, LANES)
        pair = (BLOCKS, n, 2, r, LANES)
        f32 = jnp.float32
        any_spec = pl.BlockSpec(memory_space=pl.ANY)
        smem = pl.BlockSpec(memory_space=pltpu.SMEM)
        vmem = pl.BlockSpec(memory_space=pltpu.VMEM)
        dma = pltpu.SemaphoreType.DMA
        g = len(GROUPS)
        energy, state = pl.pallas_call(
            functools.partial(kernel, layers, vregs, float(local * BLOCKS)),
            out_shape=[jax.ShapeDtypeStruct((1,), f32), pltpu.VMEM(pair, f32)],
            in_specs=[any_spec, smem, smem],
            out_specs=[smem, vmem],
            scratch_shapes=[
                pltpu.VMEM((2,) + shape, f32),
                pltpu.VMEM(pair, f32),
                pltpu.VMEM((2,) + pair, f32),
                pltpu.VMEM((2,) + pair, f32),
                pltpu.VMEM((layers, 2 * LANES, 2 * LANES), f32),
                pltpu.VMEM((layers, 2, SUBLANES, LANES), f32),
                pltpu.VMEM((SUBLANES, LANES), f32),
                pltpu.VMEM((BLOCKS, SUBLANES, LANES), f32),
                dma, dma, dma, dma((2, g)), dma((2, g)), dma, dma,
            ],
            compiler_params=pltpu.CompilerParams(collective_id=0, has_side_effects=True),
            name="qaoa",
        )(cost_local.reshape(shape), gammas, betas)
        out_re, out_im = pl.pallas_call(
            split_kernel,
            out_shape=[jax.ShapeDtypeStruct(shape, f32)] * 2,
            in_specs=[vmem],
            out_specs=[any_spec] * 2,
            scratch_shapes=[dma((2,))],
            name="split",
        )(pltpu.with_memory_space_constraint(state, pltpu.VMEM))
        return energy, out_re.reshape(local), out_im.reshape(local)

    return jax.shard_map(device_body, mesh=mesh, in_specs=(state_spec, P(), P()),
                         out_specs=(P("inst"), state_spec, state_spec), check_vma=False)
```

```python
import functools

import jax
import jax.numpy as jnp
from jax import lax
from jax.experimental import pallas as pl
from jax.experimental.pallas import tpu as pltpu
from jax.sharding import PartitionSpec as P

LANES = 128
SUBLANES = 8
BLOCKS = 16
CHUNKS = 8
GROUPS = ((0, 2), (2, 2), (4, 2), (6, 2))
GROUP = 4


def flip(x, m):
    return (x // 2 + m // 2) % 2 * 2 + (x + m) % 2


def rx_pair(a, b, c, s):
    (ar, ai), (br, bi) = a, b
    return (c * ar + s * bi, c * ai - s * br), (c * br + s * ai, c * bi - s * ar)


def rx_list(amps, c, s):
    amps = list(amps)
    step = 1
    while step < len(amps):
        for i in range(len(amps)):
            if not i & step:
                amps[i], amps[i + step] = rx_pair(amps[i], amps[i + step], c, s)
        step *= 2
    return amps


def kernel(layers, vregs, total, cost_in, gam, bet, en_out, work,
           cost, trig, recv, send, mats, tabs, en_send, en_recv, far_cost, far_send,
           load_sem, csend_sem, crecv_sem, send_sem, recv_sem, esend_sem, erecv_sem,
           fsend_sem, frecv_sem, xsend_sem, xrecv_sem, pcsend_sem, psend_sem):
    n = CHUNKS
    half = n // 2
    per = vregs // n
    a, b = lax.axis_index("qx"), lax.axis_index("qy")
    me = a * 4 + b

    def loop(lo, hi, body):
        def step(i, carry):
            body(i)
            return carry

        lax.fori_loop(lo, hi, step, 0)

    def peer(i):
        m = 15 - i
        pa, pb = flip(a, m % 4), flip(b, m // 4)
        return pa * 4 + pb, {"qx": pa, "qy": pb}

    def put(src, dst, send_s, recv_s, dev):
        return pltpu.make_async_remote_copy(src, dst, send_s, recv_s, device_id=dev,
                                            device_id_type=pl.DeviceIdType.MESH)

    load = pltpu.make_async_copy(cost_in, cost.at[0], load_sem)
    load.start()
    barrier = pltpu.get_barrier_semaphore()
    loop(0, 15, lambda i: pl.semaphore_signal(barrier, inc=1, device_id=peer(i)[1],
                                              device_id_type=pl.DeviceIdType.MESH))
    pl.semaphore_wait(barrier, 15)
    load.wait()

    half_z = b // 2
    proxy_role = (b + 1) // 2 == 1
    flips = [flip(a, m) for m in range(4)], [b, flip(b, 1)]
    near = []
    for mz, mx in ((1, 3), (1, 2), (1, 1), (1, 0), (0, 3), (0, 2), (0, 1)):
        pa, pb = flips[0][mx], flips[1][mz]
        near.append((pa * 4 + pb, {"qx": pa, "qy": pb}))

    def cross(k):
        return put(cost.at[0, :, k], far_cost.at[b % 2, :, k], xsend_sem.at[k], xrecv_sem.at[b % 2, k],
                   {"qx": a, "qy": 2 - half_z})

    cross(0).start()
    cost[1, me] = cost[0, me]

    def tables(l):
        angle = jnp.full((SUBLANES, LANES), 0.5 * bet[l], jnp.float32)
        tabs[l, 0] = jnp.cos(angle)
        tabs[l, 1] = jnp.sin(angle)
        c, s = tabs[l, 0][0:1, :], tabs[l, 1][0:1, :]
        row = lax.broadcasted_iota(jnp.int32, (LANES, LANES), 0)
        col = lax.broadcasted_iota(jnp.int32, (LANES, LANES), 1)
        size = jnp.ones((LANES, LANES), jnp.float32)
        count = jnp.zeros((LANES, LANES), jnp.int32)
        for q in range(7):
            differ = (row & (1 << q)) != (col & (1 << q))
            size = size * jnp.where(differ, s, c)
            count = count + jnp.where(differ, 1, 0)
        turn = count & 3
        m_re = jnp.where(turn == 0, size, jnp.where(turn == 2, -size, 0.0))
        m_im = jnp.where(turn == 3, size, jnp.where(turn == 1, -size, 0.0))
        mats[l, :LANES, :LANES] = m_re
        mats[l, :LANES, LANES:] = m_im
        mats[l, LANES:, :LANES] = -m_im
        mats[l, LANES:, LANES:] = m_re

    loop(0, layers, tables)

    def rows(v):
        return pl.ds(v * SUBLANES, SUBLANES)

    def take(buf, k, i, r):
        return buf[i, k, 0, r, :], buf[i, k, 1, r, :]

    def keep(buf, k, i, r, amp):
        buf[i, k, 0, r, :] = amp[0]
        buf[i, k, 1, r, :] = amp[1]

    def angles(l, src, dst, k):
        g = gam[l]

        def body(i):
            for v in range(per):
                t = g * src[i, k, rows(v), :]
                keep(dst, k, i, rows(v), (jnp.cos(t), jnp.sin(t)))

        loop(0, BLOCKS, body)

    def inner(buf, k, l):
        size = BLOCKS * per * SUBLANES
        x = jnp.concatenate([buf[:, k, 0].reshape(size, LANES), buf[:, k, 1].reshape(size, LANES)], axis=1)
        y = jnp.dot(x, mats[l], precision=lax.Precision.HIGHEST, preferred_element_type=jnp.float32)
        buf[:, k, 0] = y[:, :LANES].reshape(BLOCKS, per * SUBLANES, LANES)
        buf[:, k, 1] = y[:, LANES:].reshape(BLOCKS, per * SUBLANES, LANES)
        c, s = tabs[l, 0], tabs[l, 1]
        place = lax.broadcasted_iota(jnp.int32, (SUBLANES, LANES), 0)

        def partner(v, step):
            if 2 * step == SUBLANES:
                return pltpu.roll(v, step, 0)
            return jnp.where((place & step) != 0, pltpu.roll(v, step, 0), pltpu.roll(v, SUBLANES - step, 0))

        def body(g):
            for i in range(GROUP):
                i = g * GROUP + i
                amps = []
                for v in range(per):
                    re, im = take(buf, k, i, rows(v))
                    for step in (1, 2, 4):
                        pr, pi = partner(re, step), partner(im, step)
                        re, im = c * re + s * pi, c * im - s * pr
                    amps.append((re, im))
                for v, amp in enumerate(rx_list(amps, c, s)):
                    keep(buf, k, i, rows(v), amp)

        loop(0, BLOCKS // GROUP, body)

    def block_bits(l, k, get, dst):
        c, s = tabs[l, 0], tabs[l, 1]
        for v in range(per):
            amps = rx_list([get(i, rows(v)) for i in range(BLOCKS)], c, s)
            for i, amp in enumerate(amps):
                keep(dst, k, i, rows(v), amp)

    def chunk_pair(k0, k1, l):
        c, s = tabs[l, 0], tabs[l, 1]

        def body(i):
            for v in range(per):
                p0, p1 = rx_pair(take(work, k0, i, rows(v)), take(work, k1, i, rows(v)), c, s)
                keep(work, k0, i, rows(v), p0)
                keep(work, k1, i, rows(v), p1)

        loop(0, BLOCKS, body)

    def ship(group, p):
        lo, size = group
        part = pl.ds(lo, size)
        at = GROUPS.index(group)

        def one(i):
            j, dev = peer(i)
            put(send.at[p, j, part], recv.at[p, me, part], send_sem.at[p, at], recv_sem.at[p, at], dev).start()

        loop(0, 15, one)
        recv[p, me, part] = send[p, me, part]

    def sent(p):
        for at, (lo, size) in enumerate(GROUPS):
            part = send.at[p, pl.ds(0, BLOCKS - 1), pl.ds(lo, size)]
            pltpu.make_async_copy(part, part, send_sem.at[p, at]).wait()

    def arrived(group, p):
        lo, size = group
        part = recv.at[p, pl.ds(0, BLOCKS - 1), pl.ds(lo, size)]
        pltpu.make_async_copy(part, part, recv_sem.at[p, GROUPS.index(group)]).wait()

    def phased(k, get):
        def phased_get(i, r):
            (re, im), (co, si) = get(i, r), take(trig, k, i, r)
            return re * co + im * si, im * co - re * si

        return phased_get

    def collect(l, p):
        def fetch(k):
            block_bits(l, k, lambda i, r: take(recv.at[p], k, i, r), work)

        def early(k):
            fetch(k)
            inner(work, k, l)

        for group in GROUPS:
            lo, size = group
            hi = lo + size
            if lo in (0, half):
                pl.when(l < layers - 1)(
                    lambda: loop(lo, lo + half, lambda k: angles(l + 1, cost.at[1 - p], trig, k)))
            arrived(group, p)
            loop(lo, hi, early if hi <= half else fetch)
            if hi < n:
                chunk_pair(lo, lo + 1, l)
            if hi == half:
                loop(0, 2, lambda i: chunk_pair(i, i + 2, l))

    def first_chunk(l, k):
        c, s = tabs[l, 0], tabs[l, 1]

        def get(i, r):
            upper = rx_pair(take(work, 6 + k, i, r), take(work, 7 - k, i, r), c, s)[0]
            upper = rx_pair(take(work, 4 + k, i, r), upper, c, s)[0]
            return rx_pair(take(work, k, i, r), upper, c, s)[0]

        return get

    def rest(l):
        chunk_pair(6, 7, l)
        loop(0, 2, lambda i: chunk_pair(4 + i, 6 + i, l))

    def first(trig_ref, k):
        return lambda i, r: (trig_ref[i, k, 0, r, :], -trig_ref[i, k, 1, r, :])

    def start(k):
        for j, dev in near:
            put(cost.at[0, j, k], cost.at[1, me, k], csend_sem, crecv_sem.at[k], dev).start()
        angles(0, cost.at[0], trig, k)
        block_bits(0, k, first(trig, k), send.at[0])
        for j, dev in near:
            put(send.at[0, j, k], recv.at[0, me, k], fsend_sem.at[k], frecv_sem.at[k], dev).start()
        recv[0, me, k] = send[0, me, k]
        pl.when(k < n - 1)(lambda: cross(k + 1).start())

    def proxy(k):
        def one(x):
            s = a * 4 + 2 * (1 - half_z) + x
            pltpu.make_async_copy(far_cost.at[x, :, k], far_cost.at[x, :, k], xrecv_sem.at[x, k]).wait()
            for j, dev in near:
                put(far_cost.at[x, j, k], cost.at[1, s, k], pcsend_sem, crecv_sem.at[k], dev).start()
            pltpu.make_async_copy(far_cost.at[x, me, k], cost.at[1, s, k], crecv_sem.at[k]).start()
            angles(0, far_cost.at[x], far_send.at[x], k)
            block_bits(0, k, first(far_send.at[x], k), far_send.at[x])
            for j, dev in near:
                put(far_send.at[x, j, k], recv.at[0, s, k], psend_sem.at[k], frecv_sem.at[k], dev).start()
            pltpu.make_async_copy(far_send.at[x, me, k], recv.at[0, s, k], frecv_sem.at[k]).start()

        loop(0, 2, one)

    def first_collect(k):
        part = cost.at[0, pl.ds(0, BLOCKS - 1), k]
        pltpu.make_async_copy(part, part, crecv_sem.at[k]).wait()
        angles(1, cost.at[1], trig, k)
        part = recv.at[0, pl.ds(0, BLOCKS - 1), k]
        pltpu.make_async_copy(part, part, frecv_sem.at[k]).wait()
        block_bits(0, k, lambda i, r: take(recv.at[0], k, i, r), work)
        inner(work, k, 0)

    loop(0, n, start)

    def step(k):
        pl.when(proxy_role)(lambda: proxy(k))
        pl.when(k > 0)(lambda: first_collect(k - 1))

    loop(0, n, step)
    first_collect(n - 1)
    loop(0, 3, lambda i: chunk_pair(2 * i, 2 * i + 1, 0))
    loop(0, 2, lambda i: chunk_pair(i, i + 2, 0))

    def first_sent(k):
        pltpu.make_async_copy(cost.at[0, :, k], cost.at[0, :, k], xsend_sem.at[k]).wait()
        part = send.at[0, pl.ds(0, len(near)), k]
        pltpu.make_async_copy(part, part, fsend_sem.at[k]).wait()

    loop(0, n, first_sent)
    part = cost.at[0, pl.ds(0, len(near))]
    pltpu.make_async_copy(part, part, csend_sem).wait()

    @pl.when(proxy_role)
    def _():
        part = cost.at[0, pl.ds(0, 2 * len(near))]
        pltpu.make_async_copy(part, part, pcsend_sem).wait()

        def one(k):
            part = recv.at[0, pl.ds(0, 2 * len(near)), k]
            pltpu.make_async_copy(part, part, psend_sem.at[k]).wait()

        loop(0, n, one)

    def layer(l):
        p = l % 2
        pl.when(l > 1)(lambda: sent(1 - p))
        for group in GROUPS:
            lo, size = group
            if lo == 0:
                loop(0, 2, lambda k: block_bits(l + 1, k, phased(k, first_chunk(l, k)), send.at[1 - p]))
                ship(group, 1 - p)
                rest(l)
                loop(0, half, lambda k: chunk_pair(k, k + half, l))
                continue

            def resend(k):
                block_bits(l + 1, k, phased(k, lambda i, r: take(work, k, i, r)), send.at[1 - p])
                if lo >= half:
                    inner(send.at[1 - p], k, l + 1)

            loop(lo, lo + size, resend)
            ship(group, 1 - p)
        collect(l + 1, 1 - p)

    loop(0, layers - 1, layer)

    last = layers - 1
    rest(last)
    c, s = tabs[last, 0], tabs[last, 1]

    def finish(k, acc):
        def body(i, acc):
            for v in range(per):
                r = rows(v)
                pair = rx_pair(take(work, k, i, r), take(work, k + half, i, r), c, s)
                for kk, (re, im) in zip((k, k + half), pair):
                    keep(work, kk, i, r, (re, im))
                    acc = acc + cost[0, i, kk, r, :] * (re * re + im * im)
            return acc

        return lax.fori_loop(0, BLOCKS, body, acc)

    en_send[...] = lax.fori_loop(0, half, finish, jnp.zeros((SUBLANES, LANES), jnp.float32))
    loop(0, 15, lambda i: put(en_send, en_recv.at[me], esend_sem, erecv_sem, peer(i)[1]).start())
    en_recv[me] = en_send[...]
    part = en_recv.at[pl.ds(0, BLOCKS - 1)]
    sent(1 - last % 2)
    sent(last % 2)
    pltpu.make_async_copy(part, part, erecv_sem).wait()
    pltpu.make_async_copy(part, part, esend_sem).wait()
    full = en_recv[0]
    for i in range(1, BLOCKS):
        full = full + en_recv[i]
    en_out[0] = jnp.sum(full) / total


def split_kernel(pair, re_out, im_out, sem):
    copies = [pltpu.make_async_copy(pair.at[:, :, part], out, sem.at[part])
              for part, out in enumerate((re_out, im_out))]
    for copy in copies:
        copy.start()
    for copy in copies:
        copy.wait()


def solution(mesh):
    state_spec = P(("inst", "qx", "qy"))

    def device_body(cost_local, gammas, betas):
        local = cost_local.shape[0]
        vregs = local // (BLOCKS * SUBLANES * LANES)
        layers = gammas.shape[0]
        n = CHUNKS
        r = vregs // n * SUBLANES
        shape = (BLOCKS, n, r, LANES)
        pair = (BLOCKS, n, 2, r, LANES)
        f32 = jnp.float32
        any_spec = pl.BlockSpec(memory_space=pl.ANY)
        smem = pl.BlockSpec(memory_space=pltpu.SMEM)
        vmem = pl.BlockSpec(memory_space=pltpu.VMEM)
        dma = pltpu.SemaphoreType.DMA
        g = len(GROUPS)
        energy, state = pl.pallas_call(
            functools.partial(kernel, layers, vregs, float(local * BLOCKS)),
            out_shape=[jax.ShapeDtypeStruct((1,), f32), pltpu.VMEM(pair, f32)],
            in_specs=[any_spec, smem, smem],
            out_specs=[smem, vmem],
            scratch_shapes=[
                pltpu.VMEM((2,) + shape, f32),
                pltpu.VMEM(pair, f32),
                pltpu.VMEM((2,) + pair, f32),
                pltpu.VMEM((2,) + pair, f32),
                pltpu.VMEM((layers, 2 * LANES, 2 * LANES), f32),
                pltpu.VMEM((layers, 2, SUBLANES, LANES), f32),
                pltpu.VMEM((SUBLANES, LANES), f32),
                pltpu.VMEM((BLOCKS, SUBLANES, LANES), f32),
                pltpu.VMEM((2,) + shape, f32),
                pltpu.VMEM((2,) + pair, f32),
                dma, dma, dma((n,)), dma((2, g)), dma((2, g)), dma, dma,
                dma((n,)), dma((n,)), dma((n,)), dma((2, n)), dma, dma((n,)),
            ],
            compiler_params=pltpu.CompilerParams(collective_id=0, has_side_effects=True),
            name="qaoa",
        )(cost_local.reshape(shape), gammas, betas)
        out_re, out_im = pl.pallas_call(
            split_kernel,
            out_shape=[jax.ShapeDtypeStruct(shape, f32)] * 2,
            in_specs=[vmem],
            out_specs=[any_spec] * 2,
            scratch_shapes=[dma((2,))],
            name="split",
        )(pltpu.with_memory_space_constraint(state, pltpu.VMEM))
        return energy, out_re.reshape(local), out_im.reshape(local)

    return jax.shard_map(device_body, mesh=mesh, in_specs=(state_spec, P(), P()),
                         out_specs=(P("inst"), state_spec, state_spec), check_vma=False)
```

```python
import functools

import jax
import jax.numpy as jnp
from jax import lax
from jax.experimental import pallas as pl
from jax.experimental.pallas import tpu as pltpu
from jax.sharding import PartitionSpec as P

LANES = 128
SUBLANES = 8
BLOCKS = 16
CHUNKS = 8
GROUPS = ((0, 2), (2, 2), (4, 2), (6, 2))
GROUP = 4


def flip(x, m):
    return (x // 2 + m // 2) % 2 * 2 + (x + m) % 2


def rx_pair(a, b, c, s):
    (ar, ai), (br, bi) = a, b
    return (c * ar + s * bi, c * ai - s * br), (c * br + s * ai, c * bi - s * ar)


def rx_list(amps, c, s):
    amps = list(amps)
    step = 1
    while step < len(amps):
        for i in range(len(amps)):
            if not i & step:
                amps[i], amps[i + step] = rx_pair(amps[i], amps[i + step], c, s)
        step *= 2
    return amps


def kernel(layers, vregs, total, cost_in, gam, bet, en_out, work,
           cost, trig, recv, send, mats, tabs, en_send, en_recv, far_cost, far_send,
           load_sem, csend_sem, crecv_sem, send_sem, recv_sem, esend_sem, erecv_sem,
           fsend_sem, frecv_sem, xsend_sem, xrecv_sem, pcsend_sem, psend_sem):
    n = CHUNKS
    half = n // 2
    per = vregs // n
    a, b = lax.axis_index("qx"), lax.axis_index("qy")
    me = a * 4 + b

    def loop(lo, hi, body):
        def step(i, carry):
            body(i)
            return carry

        lax.fori_loop(lo, hi, step, 0)

    flips = [[flip(x, m) for m in range(4)] for x in (a, b)]
    peers = []
    for mz, mx in ((m // 4, m % 4) for m in range(15, 0, -1)):
        pa, pb = flips[0][mx], flips[1][mz]
        peers.append((pa * 4 + pb, {"qx": pa, "qy": pb}))
    near = peers[8:]

    def put(src, dst, send_s, recv_s, dev):
        return pltpu.make_async_remote_copy(src, dst, send_s, recv_s, device_id=dev,
                                            device_id_type=pl.DeviceIdType.MESH)

    load = pltpu.make_async_copy(cost_in, cost.at[0], load_sem)
    load.start()
    barrier = pltpu.get_barrier_semaphore()
    for _, dev in peers:
        pl.semaphore_signal(barrier, inc=1, device_id=dev, device_id_type=pl.DeviceIdType.MESH)
    pl.semaphore_wait(barrier, 15)
    load.wait()

    half_z = b // 2
    role = (b + 1) // 2 % 2
    proxy_role = role == 1
    def cross(k):
        return put(cost.at[0, :, k], far_cost.at[b % 2, :, k], xsend_sem.at[k], xrecv_sem.at[b % 2, k],
                   {"qx": a, "qy": 2 - half_z})

    cross(0).start()
    cost[1, me] = cost[0, me]

    def tables(l):
        angle = jnp.full((SUBLANES, LANES), 0.5 * bet[l], jnp.float32)
        tabs[l, 0] = jnp.cos(angle)
        tabs[l, 1] = jnp.sin(angle)
        c, s = tabs[l, 0][0:1, :], tabs[l, 1][0:1, :]
        row = lax.broadcasted_iota(jnp.int32, (LANES, LANES), 0)
        col = lax.broadcasted_iota(jnp.int32, (LANES, LANES), 1)
        size = jnp.ones((LANES, LANES), jnp.float32)
        count = jnp.zeros((LANES, LANES), jnp.int32)
        for q in range(7):
            differ = (row & (1 << q)) != (col & (1 << q))
            size = size * jnp.where(differ, s, c)
            count = count + jnp.where(differ, 1, 0)
        turn = count & 3
        m_re = jnp.where(turn == 0, size, jnp.where(turn == 2, -size, 0.0))
        m_im = jnp.where(turn == 3, size, jnp.where(turn == 1, -size, 0.0))
        mats[l, :LANES, :LANES] = m_re
        mats[l, :LANES, LANES:] = m_im
        mats[l, LANES:, :LANES] = -m_im
        mats[l, LANES:, LANES:] = m_re

    loop(0, layers, tables)

    def rows(v):
        return pl.ds(v * SUBLANES, SUBLANES)

    def take(buf, k, i, r):
        return buf[i, k, 0, r, :], buf[i, k, 1, r, :]

    def keep(buf, k, i, r, amp):
        buf[i, k, 0, r, :] = amp[0]
        buf[i, k, 1, r, :] = amp[1]

    def angles(l, src, dst, k):
        g = gam[l]

        def body(i):
            for v in range(per):
                t = g * src[i, k, rows(v), :]
                keep(dst, k, i, rows(v), (jnp.cos(t), jnp.sin(t)))

        loop(0, BLOCKS, body)

    def inner(buf, k, l):
        size = BLOCKS * per * SUBLANES
        x = jnp.concatenate([buf[:, k, 0].reshape(size, LANES), buf[:, k, 1].reshape(size, LANES)], axis=1)
        y = jnp.dot(x, mats[l], precision=lax.Precision.HIGHEST, preferred_element_type=jnp.float32)
        buf[:, k, 0] = y[:, :LANES].reshape(BLOCKS, per * SUBLANES, LANES)
        buf[:, k, 1] = y[:, LANES:].reshape(BLOCKS, per * SUBLANES, LANES)
        c, s = tabs[l, 0], tabs[l, 1]
        place = lax.broadcasted_iota(jnp.int32, (SUBLANES, LANES), 0)

        def partner(v, step):
            if 2 * step == SUBLANES:
                return pltpu.roll(v, step, 0)
            return jnp.where((place & step) != 0, pltpu.roll(v, step, 0), pltpu.roll(v, SUBLANES - step, 0))

        def body(g):
            for i in range(GROUP):
                i = g * GROUP + i
                amps = []
                for v in range(per):
                    re, im = take(buf, k, i, rows(v))
                    for step in (1, 2, 4):
                        pr, pi = partner(re, step), partner(im, step)
                        re, im = c * re + s * pi, c * im - s * pr
                    amps.append((re, im))
                for v, amp in enumerate(rx_list(amps, c, s)):
                    keep(buf, k, i, rows(v), amp)

        loop(0, BLOCKS // GROUP, body)

    def block_bits(l, k, get, dst):
        c, s = tabs[l, 0], tabs[l, 1]
        for v in range(per):
            amps = rx_list([get(i, rows(v)) for i in range(BLOCKS)], c, s)
            for i, amp in enumerate(amps):
                keep(dst, k, i, rows(v), amp)

    def chunk_pair(k0, k1, l):
        c, s = tabs[l, 0], tabs[l, 1]

        def body(i):
            for v in range(per):
                p0, p1 = rx_pair(take(work, k0, i, rows(v)), take(work, k1, i, rows(v)), c, s)
                keep(work, k0, i, rows(v), p0)
                keep(work, k1, i, rows(v), p1)

        loop(0, BLOCKS, body)

    def ship(group, p):
        lo, size = group
        part = pl.ds(lo, size)
        at = GROUPS.index(group)

        for j, dev in peers:
            put(send.at[p, j, part], recv.at[p, me, part], send_sem.at[p, at], recv_sem.at[p, at], dev).start()
        recv[p, me, part] = send[p, me, part]

    def sent(p):
        for at, (lo, size) in enumerate(GROUPS):
            part = send.at[p, pl.ds(0, BLOCKS - 1), pl.ds(lo, size)]
            pltpu.make_async_copy(part, part, send_sem.at[p, at]).wait()

    def arrived(group, p):
        lo, size = group
        part = recv.at[p, pl.ds(0, BLOCKS - 1), pl.ds(lo, size)]
        pltpu.make_async_copy(part, part, recv_sem.at[p, GROUPS.index(group)]).wait()

    def phased(k, get):
        def phased_get(i, r):
            (re, im), (co, si) = get(i, r), take(trig, k, i, r)
            return re * co + im * si, im * co - re * si

        return phased_get

    def collect(l, p):
        def fetch(k):
            block_bits(l, k, lambda i, r: take(recv.at[p], k, i, r), work)

        def early(k):
            fetch(k)
            inner(work, k, l)

        for group in GROUPS:
            lo, size = group
            hi = lo + size
            if lo in (0, half):
                pl.when(l < layers - 1)(
                    lambda: loop(lo, lo + half, lambda k: angles(l + 1, cost.at[1 - p], trig, k)))
            arrived(group, p)
            loop(lo, hi, early if hi <= half else fetch)
            if hi < n:
                chunk_pair(lo, lo + 1, l)
            if hi == half:
                loop(0, 2, lambda i: chunk_pair(i, i + 2, l))

    def first_chunk(l, k):
        c, s = tabs[l, 0], tabs[l, 1]

        def get(i, r):
            upper = rx_pair(take(work, 6 + k, i, r), take(work, 7 - k, i, r), c, s)[0]
            upper = rx_pair(take(work, 4 + k, i, r), upper, c, s)[0]
            return rx_pair(take(work, k, i, r), upper, c, s)[0]

        return get

    def rest(l):
        chunk_pair(6, 7, l)
        loop(0, 2, lambda i: chunk_pair(4 + i, 6 + i, l))

    def first(trig_ref, k):
        return lambda i, r: (trig_ref[i, k, 0, r, :], -trig_ref[i, k, 1, r, :])

    def start(k):
        for j, dev in near:
            put(cost.at[0, j, k], cost.at[1, me, k], csend_sem, crecv_sem.at[k], dev).start()
        angles(0, cost.at[0], trig, k)
        block_bits(0, k, first(trig, k), send.at[0])
        for j, dev in near:
            put(send.at[0, j, k], recv.at[0, me, k], fsend_sem.at[k], frecv_sem.at[k], dev).start()
        recv[0, me, k] = send[0, me, k]
        outer_ahead = (1 - role) * (n - 1) + role
        pl.when(k < outer_ahead)(lambda: cross(k + 1).start())

    def proxy(k):
        def one(x):
            s = a * 4 + 2 * (1 - half_z) + x
            pltpu.make_async_copy(far_cost.at[x, :, k], far_cost.at[x, :, k], xrecv_sem.at[x, k]).wait()
            for j, dev in near:
                put(far_cost.at[x, j, k], cost.at[1, s, k], pcsend_sem, crecv_sem.at[k], dev).start()
            pltpu.make_async_copy(far_cost.at[x, me, k], cost.at[1, s, k], crecv_sem.at[k]).start()
            angles(0, far_cost.at[x], far_send.at[x], k)
            block_bits(0, k, first(far_send.at[x], k), far_send.at[x])
            for j, dev in near:
                put(far_send.at[x, j, k], recv.at[0, s, k], psend_sem.at[k], frecv_sem.at[k], dev).start()
            pltpu.make_async_copy(far_send.at[x, me, k], recv.at[0, s, k], frecv_sem.at[k]).start()

        loop(0, 2, one)
        pl.when(k < n - 2)(lambda: cross(k + 2).start())

    def first_collect(k):
        part = cost.at[0, pl.ds(0, BLOCKS - 1), k]
        pltpu.make_async_copy(part, part, crecv_sem.at[k]).wait()
        angles(1, cost.at[1], trig, k)
        part = recv.at[0, pl.ds(0, BLOCKS - 1), k]
        pltpu.make_async_copy(part, part, frecv_sem.at[k]).wait()
        block_bits(0, k, lambda i, r: take(recv.at[0], k, i, r), work)
        inner(work, k, 0)

    loop(0, n, start)

    def step(k):
        pl.when(proxy_role)(lambda: proxy(k))
        pl.when(k > 0)(lambda: first_collect(k - 1))

    loop(0, n, step)
    first_collect(n - 1)
    loop(0, 3, lambda i: chunk_pair(2 * i, 2 * i + 1, 0))
    loop(0, 2, lambda i: chunk_pair(i, i + 2, 0))

    def first_sent(k):
        pltpu.make_async_copy(cost.at[0, :, k], cost.at[0, :, k], xsend_sem.at[k]).wait()
        part = send.at[0, pl.ds(0, len(near)), k]
        pltpu.make_async_copy(part, part, fsend_sem.at[k]).wait()

    loop(0, n, first_sent)
    part = cost.at[0, pl.ds(0, len(near))]
    pltpu.make_async_copy(part, part, csend_sem).wait()

    @pl.when(proxy_role)
    def _():
        part = cost.at[0, pl.ds(0, 2 * len(near))]
        pltpu.make_async_copy(part, part, pcsend_sem).wait()

        def one(k):
            part = recv.at[0, pl.ds(0, 2 * len(near)), k]
            pltpu.make_async_copy(part, part, psend_sem.at[k]).wait()

        loop(0, n, one)

    def layer(l):
        p = l % 2
        pl.when(l > 1)(lambda: sent(1 - p))
        for group in GROUPS:
            lo, size = group
            if lo == 0:
                loop(0, 2, lambda k: block_bits(l + 1, k, phased(k, first_chunk(l, k)), send.at[1 - p]))
                ship(group, 1 - p)
                rest(l)
                loop(0, half, lambda k: chunk_pair(k, k + half, l))
                continue

            def resend(k):
                block_bits(l + 1, k, phased(k, lambda i, r: take(work, k, i, r)), send.at[1 - p])
                if lo >= half:
                    inner(send.at[1 - p], k, l + 1)

            loop(lo, lo + size, resend)
            ship(group, 1 - p)
        collect(l + 1, 1 - p)

    loop(0, layers - 1, layer)

    last = layers - 1
    rest(last)
    c, s = tabs[last, 0], tabs[last, 1]

    def finish(k, acc):
        def body(i, acc):
            for v in range(per):
                r = rows(v)
                pair = rx_pair(take(work, k, i, r), take(work, k + half, i, r), c, s)
                for kk, (re, im) in zip((k, k + half), pair):
                    keep(work, kk, i, r, (re, im))
                    acc = acc + cost[0, i, kk, r, :] * (re * re + im * im)
            return acc

        return lax.fori_loop(0, BLOCKS, body, acc)

    en_send[...] = lax.fori_loop(0, half, finish, jnp.zeros((SUBLANES, LANES), jnp.float32))
    for _, dev in peers:
        put(en_send, en_recv.at[me], esend_sem, erecv_sem, dev).start()
    en_recv[me] = en_send[...]
    part = en_recv.at[pl.ds(0, BLOCKS - 1)]
    sent(1 - last % 2)
    sent(last % 2)
    pltpu.make_async_copy(part, part, erecv_sem).wait()
    pltpu.make_async_copy(part, part, esend_sem).wait()
    full = en_recv[0]
    for i in range(1, BLOCKS):
        full = full + en_recv[i]
    en_out[0] = jnp.sum(full) / total


def split_kernel(pair, re_out, im_out, sem):
    copies = [pltpu.make_async_copy(pair.at[:, :, part], out, sem.at[part])
              for part, out in enumerate((re_out, im_out))]
    for copy in copies:
        copy.start()
    for copy in copies:
        copy.wait()


def solution(mesh):
    state_spec = P(("inst", "qx", "qy"))

    def device_body(cost_local, gammas, betas):
        local = cost_local.shape[0]
        vregs = local // (BLOCKS * SUBLANES * LANES)
        layers = gammas.shape[0]
        n = CHUNKS
        r = vregs // n * SUBLANES
        shape = (BLOCKS, n, r, LANES)
        pair = (BLOCKS, n, 2, r, LANES)
        f32 = jnp.float32
        any_spec = pl.BlockSpec(memory_space=pl.ANY)
        smem = pl.BlockSpec(memory_space=pltpu.SMEM)
        vmem = pl.BlockSpec(memory_space=pltpu.VMEM)
        dma = pltpu.SemaphoreType.DMA
        g = len(GROUPS)
        energy, state = pl.pallas_call(
            functools.partial(kernel, layers, vregs, float(local * BLOCKS)),
            out_shape=[jax.ShapeDtypeStruct((1,), f32), pltpu.VMEM(pair, f32)],
            in_specs=[any_spec, smem, smem],
            out_specs=[smem, vmem],
            scratch_shapes=[
                pltpu.VMEM((2,) + shape, f32),
                pltpu.VMEM(pair, f32),
                pltpu.VMEM((2,) + pair, f32),
                pltpu.VMEM((2,) + pair, f32),
                pltpu.VMEM((layers, 2 * LANES, 2 * LANES), f32),
                pltpu.VMEM((layers, 2, SUBLANES, LANES), f32),
                pltpu.VMEM((SUBLANES, LANES), f32),
                pltpu.VMEM((BLOCKS, SUBLANES, LANES), f32),
                pltpu.VMEM((2,) + shape, f32),
                pltpu.VMEM((2,) + pair, f32),
                dma, dma, dma((n,)), dma((2, g)), dma((2, g)), dma, dma,
                dma((n,)), dma((n,)), dma((n,)), dma((2, n)), dma, dma((n,)),
            ],
            compiler_params=pltpu.CompilerParams(collective_id=0, has_side_effects=True),
            name="qaoa",
        )(cost_local.reshape(shape), gammas, betas)
        out_re, out_im = pl.pallas_call(
            split_kernel,
            out_shape=[jax.ShapeDtypeStruct(shape, f32)] * 2,
            in_specs=[vmem],
            out_specs=[any_spec] * 2,
            scratch_shapes=[dma((2,))],
            name="split",
        )(pltpu.with_memory_space_constraint(state, pltpu.VMEM))
        return energy, out_re.reshape(local), out_im.reshape(local)

    return jax.shard_map(device_body, mesh=mesh, in_specs=(state_spec, P(), P()),
                         out_specs=(P("inst"), state_spec, state_spec), check_vma=False)
```

```python
import functools

import jax
import jax.numpy as jnp
from jax import lax
from jax.experimental import pallas as pl
from jax.experimental.pallas import tpu as pltpu
from jax.sharding import PartitionSpec as P

LANES = 128
SUBLANES = 8
BLOCKS = 16
CHUNKS = 8
GROUPS = ((0, 2), (2, 2), (4, 2), (6, 2))
GROUP = 4


def flip(x, m):
    return (x // 2 + m // 2) % 2 * 2 + (x + m) % 2


def rx_pair(a, b, c, s):
    (ar, ai), (br, bi) = a, b
    return (c * ar + s * bi, c * ai - s * br), (c * br + s * ai, c * bi - s * ar)


def rx_list(amps, c, s):
    amps = list(amps)
    step = 1
    while step < len(amps):
        for i in range(len(amps)):
            if not i & step:
                amps[i], amps[i + step] = rx_pair(amps[i], amps[i + step], c, s)
        step *= 2
    return amps


def kernel(layers, vregs, total, cost_in, gam, bet, en_out, work,
           cost, trig, recv, send, mats, tabs, en_send, en_recv, far_cost, far_send,
           load_sem, csend_sem, crecv_sem, send_sem, recv_sem, esend_sem, erecv_sem,
           fsend_sem, frecv_sem, xsend_sem, xrecv_sem, pcsend_sem, psend_sem, nrecv_sem, ready_sem):
    n = CHUNKS
    half = n // 2
    per = vregs // n
    a, b = lax.axis_index("qx"), lax.axis_index("qy")
    me = a * 4 + b

    def loop(lo, hi, body):
        def step(i, carry):
            body(i)
            return carry

        lax.fori_loop(lo, hi, step, 0)

    flips = [[flip(x, m) for m in range(4)] for x in (a, b)]
    peers = []
    for mz, mx in ((m // 4, m % 4) for m in range(15, 0, -1)):
        pa, pb = flips[0][mx], flips[1][mz]
        peers.append((pa * 4 + pb, {"qx": pa, "qy": pb}))
    near = peers[8:]

    def put(src, dst, send_s, recv_s, dev):
        return pltpu.make_async_remote_copy(src, dst, send_s, recv_s, device_id=dev,
                                            device_id_type=pl.DeviceIdType.MESH)

    load = pltpu.make_async_copy(cost_in, cost.at[0], load_sem)
    load.start()
    barrier = pltpu.get_barrier_semaphore()
    half_z = b // 2
    role = (b + 1) // 2 % 2
    proxy_role = role == 1

    def signal(sem, dev):
        pl.semaphore_signal(sem, inc=1, device_id=dev, device_id_type=pl.DeviceIdType.MESH)

    for _, dev in near:
        signal(barrier, dev)
    signal(barrier, {"qx": a, "qy": 2 - half_z})
    pl.when(proxy_role)(lambda: signal(barrier, {"qx": a, "qy": 3 - 3 * half_z}))
    pl.semaphore_wait(barrier, 8 + role)
    for _, dev in near:
        signal(ready_sem, dev)
    load.wait()

    half_z = b // 2
    role = (b + 1) // 2 % 2
    proxy_role = role == 1
    def cross(k):
        return put(cost.at[0, :, k], far_cost.at[b % 2, :, k], xsend_sem.at[k], xrecv_sem.at[b % 2, k],
                   {"qx": a, "qy": 2 - half_z})

    cross(0).start()
    for j, dev in near:
        put(cost.at[0, j], cost.at[1, me], csend_sem, nrecv_sem, dev).start()
    cost[1, me] = cost[0, me]

    def tables(l):
        angle = jnp.full((SUBLANES, LANES), 0.5 * bet[l], jnp.float32)
        tabs[l, 0] = jnp.cos(angle)
        tabs[l, 1] = jnp.sin(angle)
        c, s = tabs[l, 0][0:1, :], tabs[l, 1][0:1, :]
        row = lax.broadcasted_iota(jnp.int32, (LANES, LANES), 0)
        col = lax.broadcasted_iota(jnp.int32, (LANES, LANES), 1)
        size = jnp.ones((LANES, LANES), jnp.float32)
        count = jnp.zeros((LANES, LANES), jnp.int32)
        for q in range(7):
            differ = (row & (1 << q)) != (col & (1 << q))
            size = size * jnp.where(differ, s, c)
            count = count + jnp.where(differ, 1, 0)
        turn = count & 3
        m_re = jnp.where(turn == 0, size, jnp.where(turn == 2, -size, 0.0))
        m_im = jnp.where(turn == 3, size, jnp.where(turn == 1, -size, 0.0))
        mats[l, :LANES, :LANES] = m_re
        mats[l, :LANES, LANES:] = m_im
        mats[l, LANES:, :LANES] = -m_im
        mats[l, LANES:, LANES:] = m_re

    loop(0, layers, tables)

    def rows(v):
        return pl.ds(v * SUBLANES, SUBLANES)

    def take(buf, k, i, r):
        return buf[i, k, 0, r, :], buf[i, k, 1, r, :]

    def keep(buf, k, i, r, amp):
        buf[i, k, 0, r, :] = amp[0]
        buf[i, k, 1, r, :] = amp[1]

    def angles(l, src, dst, k):
        g = gam[l]

        def body(i):
            for v in range(per):
                t = g * src[i, k, rows(v), :]
                keep(dst, k, i, rows(v), (jnp.cos(t), jnp.sin(t)))

        loop(0, BLOCKS, body)

    def inner(buf, k, l):
        size = BLOCKS * per * SUBLANES
        x = jnp.concatenate([buf[:, k, 0].reshape(size, LANES), buf[:, k, 1].reshape(size, LANES)], axis=1)
        y = jnp.dot(x, mats[l], precision=lax.Precision.HIGHEST, preferred_element_type=jnp.float32)
        buf[:, k, 0] = y[:, :LANES].reshape(BLOCKS, per * SUBLANES, LANES)
        buf[:, k, 1] = y[:, LANES:].reshape(BLOCKS, per * SUBLANES, LANES)
        c, s = tabs[l, 0], tabs[l, 1]
        place = lax.broadcasted_iota(jnp.int32, (SUBLANES, LANES), 0)

        def partner(v, step):
            if 2 * step == SUBLANES:
                return pltpu.roll(v, step, 0)
            return jnp.where((place & step) != 0, pltpu.roll(v, step, 0), pltpu.roll(v, SUBLANES - step, 0))

        def body(g):
            for i in range(GROUP):
                i = g * GROUP + i
                amps = []
                for v in range(per):
                    re, im = take(buf, k, i, rows(v))
                    for step in (1, 2, 4):
                        pr, pi = partner(re, step), partner(im, step)
                        re, im = c * re + s * pi, c * im - s * pr
                    amps.append((re, im))
                for v, amp in enumerate(rx_list(amps, c, s)):
                    keep(buf, k, i, rows(v), amp)

        loop(0, BLOCKS // GROUP, body)

    def block_bits(l, k, get, dst):
        c, s = tabs[l, 0], tabs[l, 1]
        for v in range(per):
            amps = rx_list([get(i, rows(v)) for i in range(BLOCKS)], c, s)
            for i, amp in enumerate(amps):
                keep(dst, k, i, rows(v), amp)

    def chunk_pair(k0, k1, l):
        c, s = tabs[l, 0], tabs[l, 1]

        def body(i):
            for v in range(per):
                p0, p1 = rx_pair(take(work, k0, i, rows(v)), take(work, k1, i, rows(v)), c, s)
                keep(work, k0, i, rows(v), p0)
                keep(work, k1, i, rows(v), p1)

        loop(0, BLOCKS, body)

    def ship(group, p):
        lo, size = group
        part = pl.ds(lo, size)
        at = GROUPS.index(group)

        for j, dev in peers:
            put(send.at[p, j, part], recv.at[p, me, part], send_sem.at[p, at], recv_sem.at[p, at], dev).start()
        recv[p, me, part] = send[p, me, part]

    def sent(p):
        for at, (lo, size) in enumerate(GROUPS):
            part = send.at[p, pl.ds(0, BLOCKS - 1), pl.ds(lo, size)]
            pltpu.make_async_copy(part, part, send_sem.at[p, at]).wait()

    def arrived(group, p):
        lo, size = group
        part = recv.at[p, pl.ds(0, BLOCKS - 1), pl.ds(lo, size)]
        pltpu.make_async_copy(part, part, recv_sem.at[p, GROUPS.index(group)]).wait()

    def phased(k, get):
        def phased_get(i, r):
            (re, im), (co, si) = get(i, r), take(trig, k, i, r)
            return re * co + im * si, im * co - re * si

        return phased_get

    def collect(l, p):
        def fetch(k):
            block_bits(l, k, lambda i, r: take(recv.at[p], k, i, r), work)

        def early(k):
            fetch(k)
            inner(work, k, l)

        for group in GROUPS:
            lo, size = group
            hi = lo + size
            if lo in (0, half):
                pl.when(l < layers - 1)(
                    lambda: loop(lo, lo + half, lambda k: angles(l + 1, cost.at[1 - p], trig, k)))
            arrived(group, p)
            loop(lo, hi, early if hi <= half else fetch)
            if hi < n:
                chunk_pair(lo, lo + 1, l)
            if hi == half:
                loop(0, 2, lambda i: chunk_pair(i, i + 2, l))

    def first_chunk(l, k):
        c, s = tabs[l, 0], tabs[l, 1]

        def get(i, r):
            upper = rx_pair(take(work, 6 + k, i, r), take(work, 7 - k, i, r), c, s)[0]
            upper = rx_pair(take(work, 4 + k, i, r), upper, c, s)[0]
            return rx_pair(take(work, k, i, r), upper, c, s)[0]

        return get

    def rest(l):
        chunk_pair(6, 7, l)
        loop(0, 2, lambda i: chunk_pair(4 + i, 6 + i, l))

    def first(trig_ref, k):
        return lambda i, r: (trig_ref[i, k, 0, r, :], -trig_ref[i, k, 1, r, :])

    def start(k, targets):
        if targets is peers:
            pl.semaphore_wait(ready_sem, len(near))
            for j, dev in peers[:8]:
                put(cost.at[0, j, k], cost.at[1, me, k], csend_sem, crecv_sem.at[k], dev).start()
        angles(0, cost.at[0], trig, k)
        block_bits(0, k, first(trig, k), send.at[0])
        if targets is peers:
            inner(send.at[0], k, 0)
        for j, dev in targets:
            put(send.at[0, j, k], recv.at[0, me, k], fsend_sem.at[k], frecv_sem.at[k], dev).start()
        recv[0, me, k] = send[0, me, k]

    def proxy(k):
        def one(x):
            s = a * 4 + 2 * (1 - half_z) + x
            pltpu.make_async_copy(far_cost.at[x, :, k], far_cost.at[x, :, k], xrecv_sem.at[x, k]).wait()
            for j, dev in near:
                put(far_cost.at[x, j, k], cost.at[1, s, k], pcsend_sem, crecv_sem.at[k], dev).start()
            pltpu.make_async_copy(far_cost.at[x, me, k], cost.at[1, s, k], crecv_sem.at[k]).start()
            angles(0, far_cost.at[x], far_send.at[x], k)
            block_bits(0, k, first(far_send.at[x], k), far_send.at[x])
            for j, dev in near:
                put(far_send.at[x, j, k], recv.at[0, s, k], psend_sem.at[k], frecv_sem.at[k], dev).start()
            pltpu.make_async_copy(far_send.at[x, me, k], recv.at[0, s, k], frecv_sem.at[k]).start()

        loop(0, 2, one)

    def first_collect(k, last=False):
        part = cost.at[0, pl.ds(0, 8), k]
        pltpu.make_async_copy(part, part, crecv_sem.at[k]).wait()
        angles(1, cost.at[1], trig, k)
        if last:
            chunk_pair(4, 5, 0)
            loop(0, 2, lambda i: chunk_pair(2 * i, 2 * i + 1, 0))
            loop(0, 2, lambda i: chunk_pair(i, i + 2, 0))
        part = recv.at[0, pl.ds(0, BLOCKS - 1), k]
        pltpu.make_async_copy(part, part, frecv_sem.at[k]).wait()
        block_bits(0, k, lambda i, r: take(recv.at[0], k, i, r), work)
        if not last:
            inner(work, k, 0)

    def begin(k):
        start(k, near)
        pl.when(k < n - 2)(lambda: cross(k + 1).start())

    loop(0, n - 1, begin)
    start(n - 1, peers)

    def step(k):
        pl.when(proxy_role)(lambda: proxy(k))

        @pl.when(k == 1)
        def _():
            part = cost.at[0, pl.ds(0, len(near))]
            pltpu.make_async_copy(part, part, nrecv_sem).wait()

        pl.when(k > 0)(lambda: first_collect(k - 1))

    loop(0, n - 1, step)
    first_collect(n - 2)
    first_collect(n - 1, True)

    def first_sent(k):
        pltpu.make_async_copy(cost.at[0, :, k], cost.at[0, :, k], xsend_sem.at[k]).wait()
        part = send.at[0, pl.ds(0, len(near)), k]
        pltpu.make_async_copy(part, part, fsend_sem.at[k]).wait()

    loop(0, n - 1, first_sent)
    part = send.at[0, pl.ds(0, len(peers)), n - 1]
    pltpu.make_async_copy(part, part, fsend_sem.at[n - 1]).wait()
    part = cost.at[0, pl.ds(0, (len(near) * (n - 1) + len(peers)) // n)]
    pltpu.make_async_copy(part, part, csend_sem).wait()

    @pl.when(proxy_role)
    def _():
        part = cost.at[0, pl.ds(0, 2 * len(near)), pl.ds(0, n - 1)]
        pltpu.make_async_copy(part, part, pcsend_sem).wait()

        def one(k):
            part = recv.at[0, pl.ds(0, 2 * len(near)), k]
            pltpu.make_async_copy(part, part, psend_sem.at[k]).wait()

        loop(0, n - 1, one)

    def layer(l):
        p = l % 2
        pl.when(l > 1)(lambda: sent(1 - p))
        for group in GROUPS:
            lo, size = group
            if lo == 0:
                loop(0, 2, lambda k: block_bits(l + 1, k, phased(k, first_chunk(l, k)), send.at[1 - p]))
                ship(group, 1 - p)
                rest(l)
                loop(0, half, lambda k: chunk_pair(k, k + half, l))
                continue

            def resend(k):
                block_bits(l + 1, k, phased(k, lambda i, r: take(work, k, i, r)), send.at[1 - p])
                if lo >= half:
                    inner(send.at[1 - p], k, l + 1)

            loop(lo, lo + size, resend)
            ship(group, 1 - p)
        collect(l + 1, 1 - p)

    loop(0, layers - 1, layer)

    last = layers - 1
    c, s = tabs[last, 0], tabs[last, 1]

    def finish(i, acc):
        for v in range(per):
            r = rows(v)
            amps = [take(work, k, i, r) for k in range(n)]
            for k0, k1 in ((6, 7), (4, 6), (5, 7), (0, 4), (1, 5), (2, 6), (3, 7)):
                amps[k0], amps[k1] = rx_pair(amps[k0], amps[k1], c, s)
            for k, (re, im) in enumerate(amps):
                keep(work, k, i, r, (re, im))
                acc = acc + cost[0, i, k, r, :] * (re * re + im * im)
        return acc

    en_send[...] = lax.fori_loop(0, BLOCKS, finish, jnp.zeros((SUBLANES, LANES), jnp.float32))
    for _, dev in peers:
        put(en_send, en_recv.at[me], esend_sem, erecv_sem, dev).start()
    en_recv[me] = en_send[...]
    part = en_recv.at[pl.ds(0, BLOCKS - 1)]
    sent(1 - last % 2)
    sent(last % 2)
    pltpu.make_async_copy(part, part, erecv_sem).wait()
    pltpu.make_async_copy(part, part, esend_sem).wait()
    full = en_recv[0]
    for i in range(1, BLOCKS):
        full = full + en_recv[i]
    en_out[0] = jnp.sum(full) / total


def split_kernel(pair, re_out, im_out, sem):
    copies = [pltpu.make_async_copy(pair.at[:, :, part], out, sem.at[part])
              for part, out in enumerate((re_out, im_out))]
    for copy in copies:
        copy.start()
    for copy in copies:
        copy.wait()


def solution(mesh):
    state_spec = P(("inst", "qx", "qy"))

    def device_body(cost_local, gammas, betas):
        local = cost_local.shape[0]
        vregs = local // (BLOCKS * SUBLANES * LANES)
        layers = gammas.shape[0]
        n = CHUNKS
        r = vregs // n * SUBLANES
        shape = (BLOCKS, n, r, LANES)
        pair = (BLOCKS, n, 2, r, LANES)
        f32 = jnp.float32
        any_spec = pl.BlockSpec(memory_space=pl.ANY)
        smem = pl.BlockSpec(memory_space=pltpu.SMEM)
        vmem = pl.BlockSpec(memory_space=pltpu.VMEM)
        dma = pltpu.SemaphoreType.DMA
        g = len(GROUPS)
        energy, state = pl.pallas_call(
            functools.partial(kernel, layers, vregs, float(local * BLOCKS)),
            out_shape=[jax.ShapeDtypeStruct((1,), f32), pltpu.VMEM(pair, f32)],
            in_specs=[any_spec, smem, smem],
            out_specs=[smem, vmem],
            scratch_shapes=[
                pltpu.VMEM((2,) + shape, f32),
                pltpu.VMEM(pair, f32),
                pltpu.VMEM((2,) + pair, f32),
                pltpu.VMEM((2,) + pair, f32),
                pltpu.VMEM((layers, 2 * LANES, 2 * LANES), f32),
                pltpu.VMEM((layers, 2, SUBLANES, LANES), f32),
                pltpu.VMEM((SUBLANES, LANES), f32),
                pltpu.VMEM((BLOCKS, SUBLANES, LANES), f32),
                pltpu.VMEM((2,) + shape, f32),
                pltpu.VMEM((2,) + pair, f32),
                dma, dma, dma((n,)), dma((2, g)), dma((2, g)), dma, dma,
                dma((n,)), dma((n,)), dma((n,)), dma((2, n)), dma, dma((n,)), dma,
                pltpu.SemaphoreType.REGULAR,
            ],
            compiler_params=pltpu.CompilerParams(collective_id=0, has_side_effects=True),
            name="qaoa",
        )(cost_local.reshape(shape), gammas, betas)
        out_re, out_im = pl.pallas_call(
            split_kernel,
            out_shape=[jax.ShapeDtypeStruct(shape, f32)] * 2,
            in_specs=[vmem],
            out_specs=[any_spec] * 2,
            scratch_shapes=[dma((2,))],
            name="split",
        )(pltpu.with_memory_space_constraint(state, pltpu.VMEM))
        return energy, out_re.reshape(local), out_im.reshape(local)

    return jax.shard_map(device_body, mesh=mesh, in_specs=(state_spec, P(), P()),
                         out_specs=(P("inst"), state_spec, state_spec), check_vma=False)
```

```python
import functools

import jax
import jax.numpy as jnp
from jax import lax
from jax.experimental import pallas as pl
from jax.experimental.pallas import tpu as pltpu
from jax.sharding import PartitionSpec as P

LANES = 128
SUBLANES = 8
BLOCKS = 16
CHUNKS = 8
GROUPS = ((0, 2), (2, 2), (4, 2), (6, 2))
GROUP = 4


def flip(x, m):
    return (x // 2 + m // 2) % 2 * 2 + (x + m) % 2


def rx_pair(a, b, c, s):
    (ar, ai), (br, bi) = a, b
    return (c * ar + s * bi, c * ai - s * br), (c * br + s * ai, c * bi - s * ar)


def rx_list(amps, c, s):
    amps = list(amps)
    step = 1
    while step < len(amps):
        for i in range(len(amps)):
            if not i & step:
                amps[i], amps[i + step] = rx_pair(amps[i], amps[i + step], c, s)
        step *= 2
    return amps


def kernel(layers, vregs, total, cost_in, gam, bet, en_out, work,
           cost, trig, recv, send, mats, tabs, en_send, en_recv, far_cost, far_send,
           load_sem, csend_sem, crecv_sem, send_sem, recv_sem, esend_sem, erecv_sem,
           fsend_sem, frecv_sem, xsend_sem, xrecv_sem, pcsend_sem, psend_sem, nrecv_sem, ready_sem):
    n = CHUNKS
    half = n // 2
    per = vregs // n
    a, b = lax.axis_index("qx"), lax.axis_index("qy")
    me = a * 4 + b

    def loop(lo, hi, body):
        def step(i, carry):
            body(i)
            return carry

        lax.fori_loop(lo, hi, step, 0)

    flips = [[flip(x, m) for m in range(4)] for x in (a, b)]
    peers = []
    for mz, mx in ((m // 4, m % 4) for m in range(15, 0, -1)):
        pa, pb = flips[0][mx], flips[1][mz]
        peers.append((pa * 4 + pb, {"qx": pa, "qy": pb}))
    near = peers[8:]

    def put(src, dst, send_s, recv_s, dev):
        return pltpu.make_async_remote_copy(src, dst, send_s, recv_s, device_id=dev,
                                            device_id_type=pl.DeviceIdType.MESH)

    load = pltpu.make_async_copy(cost_in, cost.at[0], load_sem)
    load.start()
    barrier = pltpu.get_barrier_semaphore()
    half_z = b // 2
    role = (b + 1) // 2 % 2
    proxy_role = role == 1

    def signal(sem, dev):
        pl.semaphore_signal(sem, inc=1, device_id=dev, device_id_type=pl.DeviceIdType.MESH)

    for _, dev in near:
        signal(barrier, dev)
    signal(barrier, {"qx": a, "qy": 2 - half_z})
    pl.when(proxy_role)(lambda: signal(barrier, {"qx": a, "qy": 3 - 3 * half_z}))
    pl.semaphore_wait(barrier, 8 + role)
    for _, dev in near:
        signal(ready_sem, dev)
    load.wait()

    half_z = b // 2
    role = (b + 1) // 2 % 2
    proxy_role = role == 1
    def cross(k):
        return put(cost.at[0, :, k], far_cost.at[b % 2, :, k], xsend_sem.at[k], xrecv_sem.at[b % 2, k],
                   {"qx": a, "qy": 2 - half_z})

    cross(0).start()
    for j, dev in near:
        put(cost.at[0, j], cost.at[1, me], csend_sem, nrecv_sem, dev).start()
    cost[1, me] = cost[0, me]

    def tables(l):
        angle = jnp.full((SUBLANES, LANES), 0.5 * bet[l], jnp.float32)
        tabs[l, 0] = jnp.cos(angle)
        tabs[l, 1] = jnp.sin(angle)
        c, s = tabs[l, 0][0:1, :], tabs[l, 1][0:1, :]
        row = lax.broadcasted_iota(jnp.int32, (LANES, LANES), 0)
        col = lax.broadcasted_iota(jnp.int32, (LANES, LANES), 1)
        size = jnp.ones((LANES, LANES), jnp.float32)
        count = jnp.zeros((LANES, LANES), jnp.int32)
        for q in range(7):
            differ = (row & (1 << q)) != (col & (1 << q))
            size = size * jnp.where(differ, s, c)
            count = count + jnp.where(differ, 1, 0)
        turn = count & 3
        m_re = jnp.where(turn == 0, size, jnp.where(turn == 2, -size, 0.0))
        m_im = jnp.where(turn == 3, size, jnp.where(turn == 1, -size, 0.0))
        mats[l, :LANES, :LANES] = m_re
        mats[l, :LANES, LANES:] = m_im
        mats[l, LANES:, :LANES] = -m_im
        mats[l, LANES:, LANES:] = m_re

    loop(0, layers, tables)

    def rows(v):
        return pl.ds(v * SUBLANES, SUBLANES)

    def take(buf, k, i, r):
        if buf is work:
            return buf[0, i, k, r, :], buf[1, i, k, r, :]
        return buf[i, k, 0, r, :], buf[i, k, 1, r, :]

    def keep(buf, k, i, r, amp):
        for part in range(2):
            if buf is work:
                buf[part, i, k, r, :] = amp[part]
            else:
                buf[i, k, part, r, :] = amp[part]

    def angles(l, src, dst, k):
        g = gam[l]

        def body(i):
            for v in range(per):
                t = g * src[i, k, rows(v), :]
                keep(dst, k, i, rows(v), (jnp.cos(t), jnp.sin(t)))

        loop(0, BLOCKS, body)

    def inner(buf, k, l):
        size = BLOCKS * per * SUBLANES
        re_at, im_at = [(part, slice(None), k) if buf is work else (slice(None), k, part) for part in range(2)]
        x = jnp.concatenate([buf[re_at].reshape(size, LANES), buf[im_at].reshape(size, LANES)], axis=1)
        y = jnp.dot(x, mats[l], precision=lax.Precision.HIGHEST, preferred_element_type=jnp.float32)
        buf[re_at] = y[:, :LANES].reshape(BLOCKS, per * SUBLANES, LANES)
        buf[im_at] = y[:, LANES:].reshape(BLOCKS, per * SUBLANES, LANES)
        c, s = tabs[l, 0], tabs[l, 1]
        place = lax.broadcasted_iota(jnp.int32, (SUBLANES, LANES), 0)

        def partner(v, step):
            if 2 * step == SUBLANES:
                return pltpu.roll(v, step, 0)
            return jnp.where((place & step) != 0, pltpu.roll(v, step, 0), pltpu.roll(v, SUBLANES - step, 0))

        def body(g):
            for i in range(GROUP):
                i = g * GROUP + i
                amps = []
                for v in range(per):
                    re, im = take(buf, k, i, rows(v))
                    for step in (1, 2, 4):
                        pr, pi = partner(re, step), partner(im, step)
                        re, im = c * re + s * pi, c * im - s * pr
                    amps.append((re, im))
                for v, amp in enumerate(rx_list(amps, c, s)):
                    keep(buf, k, i, rows(v), amp)

        loop(0, BLOCKS // GROUP, body)

    def block_bits(l, k, get, dst):
        c, s = tabs[l, 0], tabs[l, 1]
        for v in range(per):
            amps = rx_list([get(i, rows(v)) for i in range(BLOCKS)], c, s)
            for i, amp in enumerate(amps):
                keep(dst, k, i, rows(v), amp)

    def chunk_pair(k0, k1, l):
        c, s = tabs[l, 0], tabs[l, 1]

        def body(i):
            for v in range(per):
                p0, p1 = rx_pair(take(work, k0, i, rows(v)), take(work, k1, i, rows(v)), c, s)
                keep(work, k0, i, rows(v), p0)
                keep(work, k1, i, rows(v), p1)

        loop(0, BLOCKS, body)

    def ship(group, p):
        lo, size = group
        part = pl.ds(lo, size)
        at = GROUPS.index(group)

        for j, dev in peers:
            put(send.at[p, j, part], recv.at[p, me, part], send_sem.at[p, at], recv_sem.at[p, at], dev).start()
        recv[p, me, part] = send[p, me, part]

    def sent(p):
        for at, (lo, size) in enumerate(GROUPS):
            part = send.at[p, pl.ds(0, BLOCKS - 1), pl.ds(lo, size)]
            pltpu.make_async_copy(part, part, send_sem.at[p, at]).wait()

    def arrived(group, p):
        lo, size = group
        part = recv.at[p, pl.ds(0, BLOCKS - 1), pl.ds(lo, size)]
        pltpu.make_async_copy(part, part, recv_sem.at[p, GROUPS.index(group)]).wait()

    def phased(k, get):
        def phased_get(i, r):
            (re, im), (co, si) = get(i, r), take(trig, k, i, r)
            return re * co + im * si, im * co - re * si

        return phased_get

    def collect(l, p):
        def fetch(k):
            block_bits(l, k, lambda i, r: take(recv.at[p], k, i, r), work)

        def early(k):
            fetch(k)
            inner(work, k, l)

        for group in GROUPS:
            lo, size = group
            hi = lo + size
            if lo in (0, half):
                pl.when(l < layers - 1)(
                    lambda: loop(lo, lo + half, lambda k: angles(l + 1, cost.at[1 - p], trig, k)))
            arrived(group, p)
            loop(lo, hi, early if hi <= half else fetch)
            if hi < n:
                chunk_pair(lo, lo + 1, l)
            if hi == half:
                loop(0, 2, lambda i: chunk_pair(i, i + 2, l))

    def first_chunk(l, k):
        c, s = tabs[l, 0], tabs[l, 1]

        def get(i, r):
            upper = rx_pair(take(work, 6 + k, i, r), take(work, 7 - k, i, r), c, s)[0]
            upper = rx_pair(take(work, 4 + k, i, r), upper, c, s)[0]
            return rx_pair(take(work, k, i, r), upper, c, s)[0]

        return get

    def rest(l):
        chunk_pair(6, 7, l)
        loop(0, 2, lambda i: chunk_pair(4 + i, 6 + i, l))

    def first(trig_ref, k):
        return lambda i, r: (trig_ref[i, k, 0, r, :], -trig_ref[i, k, 1, r, :])

    def start(k, targets):
        if targets is peers:
            pl.semaphore_wait(ready_sem, len(near))
            for j, dev in peers[:8]:
                put(cost.at[0, j, k], cost.at[1, me, k], csend_sem, crecv_sem.at[k], dev).start()
        angles(0, cost.at[0], trig, k)
        block_bits(0, k, first(trig, k), send.at[0])
        if targets is peers:
            inner(send.at[0], k, 0)
        for j, dev in targets:
            put(send.at[0, j, k], recv.at[0, me, k], fsend_sem.at[k], frecv_sem.at[k], dev).start()
        recv[0, me, k] = send[0, me, k]

    def proxy(k):
        def one(x):
            s = a * 4 + 2 * (1 - half_z) + x
            pltpu.make_async_copy(far_cost.at[x, :, k], far_cost.at[x, :, k], xrecv_sem.at[x, k]).wait()
            for j, dev in near:
                put(far_cost.at[x, j, k], cost.at[1, s, k], pcsend_sem, crecv_sem.at[k], dev).start()
            pltpu.make_async_copy(far_cost.at[x, me, k], cost.at[1, s, k], crecv_sem.at[k]).start()
            angles(0, far_cost.at[x], far_send.at[x], k)
            block_bits(0, k, first(far_send.at[x], k), far_send.at[x])
            for j, dev in near:
                put(far_send.at[x, j, k], recv.at[0, s, k], psend_sem.at[k], frecv_sem.at[k], dev).start()
            pltpu.make_async_copy(far_send.at[x, me, k], recv.at[0, s, k], frecv_sem.at[k]).start()

        loop(0, 2, one)

    def first_collect(k, last=False):
        part = cost.at[0, pl.ds(0, 8), k]
        pltpu.make_async_copy(part, part, crecv_sem.at[k]).wait()
        angles(1, cost.at[1], trig, k)
        if last:
            chunk_pair(4, 5, 0)
            loop(0, 2, lambda i: chunk_pair(2 * i, 2 * i + 1, 0))
            loop(0, 2, lambda i: chunk_pair(i, i + 2, 0))
        part = recv.at[0, pl.ds(0, BLOCKS - 1), k]
        pltpu.make_async_copy(part, part, frecv_sem.at[k]).wait()
        block_bits(0, k, lambda i, r: take(recv.at[0], k, i, r), work)
        if not last:
            inner(work, k, 0)

    def begin(k):
        start(k, near)
        pl.when(k < n - 2)(lambda: cross(k + 1).start())

    loop(0, n - 1, begin)
    start(n - 1, peers)

    def step(k):
        pl.when(proxy_role)(lambda: proxy(k))

        @pl.when(k == 1)
        def _():
            part = cost.at[0, pl.ds(0, len(near))]
            pltpu.make_async_copy(part, part, nrecv_sem).wait()

        pl.when(k > 0)(lambda: first_collect(k - 1))

    loop(0, n - 1, step)
    first_collect(n - 2)
    first_collect(n - 1, True)

    def first_sent(k):
        pltpu.make_async_copy(cost.at[0, :, k], cost.at[0, :, k], xsend_sem.at[k]).wait()
        part = send.at[0, pl.ds(0, len(near)), k]
        pltpu.make_async_copy(part, part, fsend_sem.at[k]).wait()

    def first_sends():
        loop(0, n - 1, first_sent)
        part = send.at[0, pl.ds(0, len(peers)), n - 1]
        pltpu.make_async_copy(part, part, fsend_sem.at[n - 1]).wait()
        part = cost.at[0, pl.ds(0, (len(near) * (n - 1) + len(peers)) // n)]
        pltpu.make_async_copy(part, part, csend_sem).wait()

        @pl.when(proxy_role)
        def _():
            part = cost.at[0, pl.ds(0, 2 * len(near)), pl.ds(0, n - 1)]
            pltpu.make_async_copy(part, part, pcsend_sem).wait()

            def one(k):
                part = recv.at[0, pl.ds(0, 2 * len(near)), k]
                pltpu.make_async_copy(part, part, psend_sem.at[k]).wait()

            loop(0, n - 1, one)

    def layer(l):
        p = l % 2
        pl.when(l == 1)(first_sends)
        pl.when(l > 1)(lambda: sent(1 - p))
        for group in GROUPS:
            lo, size = group
            if lo == 0:
                loop(0, 2, lambda k: block_bits(l + 1, k, phased(k, first_chunk(l, k)), send.at[1 - p]))
                ship(group, 1 - p)
                rest(l)
                loop(0, half, lambda k: chunk_pair(k, k + half, l))
                continue

            def resend(k):
                block_bits(l + 1, k, phased(k, lambda i, r: take(work, k, i, r)), send.at[1 - p])
                if lo >= half:
                    inner(send.at[1 - p], k, l + 1)

            loop(lo, lo + size, resend)
            ship(group, 1 - p)
        collect(l + 1, 1 - p)

    loop(0, layers - 1, layer)

    last = layers - 1
    c, s = tabs[last, 0], tabs[last, 1]

    def finish(i, acc):
        for v in range(per):
            r = rows(v)
            amps = [take(work, k, i, r) for k in range(n)]
            for k0, k1 in ((6, 7), (4, 6), (5, 7), (0, 4), (1, 5), (2, 6), (3, 7)):
                amps[k0], amps[k1] = rx_pair(amps[k0], amps[k1], c, s)
            for k, (re, im) in enumerate(amps):
                keep(work, k, i, r, (re, im))
                acc = acc + cost[0, i, k, r, :] * (re * re + im * im)
        return acc

    en_send[...] = lax.fori_loop(0, BLOCKS, finish, jnp.zeros((SUBLANES, LANES), jnp.float32))
    for _, dev in peers:
        put(en_send, en_recv.at[me], esend_sem, erecv_sem, dev).start()
    en_recv[me] = en_send[...]
    part = en_recv.at[pl.ds(0, BLOCKS - 1)]
    sent(1 - last % 2)
    sent(last % 2)
    pltpu.make_async_copy(part, part, erecv_sem).wait()
    pltpu.make_async_copy(part, part, esend_sem).wait()
    full = en_recv[0]
    for i in range(1, BLOCKS):
        full = full + en_recv[i]
    en_out[0] = jnp.sum(full) / total


def split_kernel(pair, re_out, im_out, sem):
    copies = [pltpu.make_async_copy(pair.at[part], out, sem.at[part])
              for part, out in enumerate((re_out, im_out))]
    for copy in copies:
        copy.start()
    for copy in copies:
        copy.wait()


def solution(mesh):
    state_spec = P(("inst", "qx", "qy"))

    def device_body(cost_local, gammas, betas):
        local = cost_local.shape[0]
        vregs = local // (BLOCKS * SUBLANES * LANES)
        layers = gammas.shape[0]
        n = CHUNKS
        r = vregs // n * SUBLANES
        shape = (BLOCKS, n, r, LANES)
        pair = (BLOCKS, n, 2, r, LANES)
        f32 = jnp.float32
        any_spec = pl.BlockSpec(memory_space=pl.ANY)
        smem = pl.BlockSpec(memory_space=pltpu.SMEM)
        vmem = pl.BlockSpec(memory_space=pltpu.VMEM)
        dma = pltpu.SemaphoreType.DMA
        g = len(GROUPS)
        energy, state = pl.pallas_call(
            functools.partial(kernel, layers, vregs, float(local * BLOCKS)),
            out_shape=[jax.ShapeDtypeStruct((1,), f32), pltpu.VMEM((2,) + shape, f32)],
            in_specs=[any_spec, smem, smem],
            out_specs=[smem, vmem],
            scratch_shapes=[
                pltpu.VMEM((2,) + shape, f32),
                pltpu.VMEM(pair, f32),
                pltpu.VMEM((2,) + pair, f32),
                pltpu.VMEM((2,) + pair, f32),
                pltpu.VMEM((layers, 2 * LANES, 2 * LANES), f32),
                pltpu.VMEM((layers, 2, SUBLANES, LANES), f32),
                pltpu.VMEM((SUBLANES, LANES), f32),
                pltpu.VMEM((BLOCKS, SUBLANES, LANES), f32),
                pltpu.VMEM((2,) + shape, f32),
                pltpu.VMEM((2,) + pair, f32),
                dma, dma, dma((n,)), dma((2, g)), dma((2, g)), dma, dma,
                dma((n,)), dma((n,)), dma((n,)), dma((2, n)), dma, dma((n,)), dma,
                pltpu.SemaphoreType.REGULAR,
            ],
            compiler_params=pltpu.CompilerParams(collective_id=0, has_side_effects=True),
            name="qaoa",
        )(cost_local.reshape(shape), gammas, betas)
        out_re, out_im = pl.pallas_call(
            split_kernel,
            out_shape=[jax.ShapeDtypeStruct(shape, f32)] * 2,
            in_specs=[vmem],
            out_specs=[any_spec] * 2,
            scratch_shapes=[dma((2,))],
            name="split",
        )(pltpu.with_memory_space_constraint(state, pltpu.VMEM))
        return energy, out_re.reshape(local), out_im.reshape(local)

    return jax.shard_map(device_body, mesh=mesh, in_specs=(state_spec, P(), P()),
                         out_specs=(P("inst"), state_spec, state_spec), check_vma=False)
```

```python
import functools

import jax
import jax.numpy as jnp
from jax import lax
from jax.experimental import pallas as pl
from jax.experimental.pallas import tpu as pltpu
from jax.sharding import PartitionSpec as P

LANES = 128
SUBLANES = 8
BLOCKS = 16
CHUNKS = 8
GROUPS = ((0, 2), (2, 2), (4, 2), (6, 2))
GROUP = 4


def flip(x, m):
    return (x // 2 + m // 2) % 2 * 2 + (x + m) % 2


def rx_pair(a, b, c, s):
    (ar, ai), (br, bi) = a, b
    return (c * ar + s * bi, c * ai - s * br), (c * br + s * ai, c * bi - s * ar)


def rx_list(amps, c, s):
    amps = list(amps)
    step = 1
    while step < len(amps):
        for i in range(len(amps)):
            if not i & step:
                amps[i], amps[i + step] = rx_pair(amps[i], amps[i + step], c, s)
        step *= 2
    return amps


def kernel(layers, vregs, total, cost_in, gam, bet, en_out, work,
           cost, trig, recv, send, mats, tabs, en_send, en_recv, far_cost, far_send,
           load_sem, csend_sem, crecv_sem, send_sem, recv_sem, esend_sem, erecv_sem,
           fsend_sem, frecv_sem, xsend_sem, xrecv_sem, pcsend_sem, psend_sem, nrecv_sem, ready_sem):
    n = CHUNKS
    half = n // 2
    per = vregs // n
    a, b = lax.axis_index("qx"), lax.axis_index("qy")
    me = a * 4 + b

    def loop(lo, hi, body):
        def step(i, carry):
            body(i)
            return carry

        lax.fori_loop(lo, hi, step, 0)

    flips = [[flip(x, m) for m in range(4)] for x in (a, b)]
    peers = []
    for mz, mx in ((m // 4, m % 4) for m in range(15, 0, -1)):
        pa, pb = flips[0][mx], flips[1][mz]
        peers.append((pa * 4 + pb, {"qx": pa, "qy": pb}))
    near = peers[8:]

    def put(src, dst, send_s, recv_s, dev):
        return pltpu.make_async_remote_copy(src, dst, send_s, recv_s, device_id=dev,
                                            device_id_type=pl.DeviceIdType.MESH)

    load = pltpu.make_async_copy(cost_in, cost.at[0], load_sem)
    load.start()
    barrier = pltpu.get_barrier_semaphore()
    half_z = b // 2
    role = (b + 1) // 2 % 2
    proxy_role = role == 1

    def signal(sem, dev):
        pl.semaphore_signal(sem, inc=1, device_id=dev, device_id_type=pl.DeviceIdType.MESH)

    for _, dev in near:
        signal(barrier, dev)
    signal(barrier, {"qx": a, "qy": 2 - half_z})
    pl.when(proxy_role)(lambda: signal(barrier, {"qx": a, "qy": 3 - 3 * half_z}))
    pl.semaphore_wait(barrier, 8 + role)
    for _, dev in near:
        signal(ready_sem, dev)
    load.wait()

    half_z = b // 2
    role = (b + 1) // 2 % 2
    proxy_role = role == 1
    def cross(k):
        return put(cost.at[0, :, k], far_cost.at[b % 2, :, k], xsend_sem.at[k], xrecv_sem.at[b % 2, k],
                   {"qx": a, "qy": 2 - half_z})

    cross(0).start()
    for j, dev in near:
        put(cost.at[0, j], cost.at[1, me], csend_sem, nrecv_sem, dev).start()
    cost[1, me] = cost[0, me]

    def tables(l):
        angle = jnp.full((SUBLANES, LANES), 0.5 * bet[l], jnp.float32)
        tabs[l, 0] = jnp.cos(angle)
        tabs[l, 1] = jnp.sin(angle)
        c, s = tabs[l, 0][0:1, :], tabs[l, 1][0:1, :]
        row = lax.broadcasted_iota(jnp.int32, (LANES, LANES), 0)
        col = lax.broadcasted_iota(jnp.int32, (LANES, LANES), 1)
        size = jnp.ones((LANES, LANES), jnp.float32)
        count = jnp.zeros((LANES, LANES), jnp.int32)
        for q in range(7):
            differ = (row & (1 << q)) != (col & (1 << q))
            size = size * jnp.where(differ, s, c)
            count = count + jnp.where(differ, 1, 0)
        turn = count & 3
        m_re = jnp.where(turn == 0, size, jnp.where(turn == 2, -size, 0.0))
        m_im = jnp.where(turn == 3, size, jnp.where(turn == 1, -size, 0.0))
        mats[l, :LANES, :LANES] = m_re
        mats[l, :LANES, LANES:] = m_im
        mats[l, LANES:, :LANES] = -m_im
        mats[l, LANES:, LANES:] = m_re

    loop(0, layers, tables)

    def rows(v):
        return pl.ds(v * SUBLANES, SUBLANES)

    def take(buf, k, i, r):
        if buf is work:
            return buf[0, i, k, r, :], buf[1, i, k, r, :]
        return buf[i, k, 0, r, :], buf[i, k, 1, r, :]

    def keep(buf, k, i, r, amp):
        for part in range(2):
            if buf is work:
                buf[part, i, k, r, :] = amp[part]
            else:
                buf[i, k, part, r, :] = amp[part]

    def angles(l, src, dst, k):
        g = gam[l]

        def body(i):
            for v in range(per):
                t = g * src[i, k, rows(v), :]
                keep(dst, k, i, rows(v), (jnp.cos(t), jnp.sin(t)))

        loop(0, BLOCKS, body)

    def inner(buf, k, l):
        size = BLOCKS * per * SUBLANES
        re_at, im_at = [(part, slice(None), k) if buf is work else (slice(None), k, part) for part in range(2)]
        x = jnp.concatenate([buf[re_at].reshape(size, LANES), buf[im_at].reshape(size, LANES)], axis=1)
        y = jnp.dot(x, mats[l], precision=lax.Precision.HIGHEST, preferred_element_type=jnp.float32)
        buf[re_at] = y[:, :LANES].reshape(BLOCKS, per * SUBLANES, LANES)
        buf[im_at] = y[:, LANES:].reshape(BLOCKS, per * SUBLANES, LANES)
        c, s = tabs[l, 0], tabs[l, 1]
        place = lax.broadcasted_iota(jnp.int32, (SUBLANES, LANES), 0)

        def partner(v, step):
            if 2 * step == SUBLANES:
                return pltpu.roll(v, step, 0)
            return jnp.where((place & step) != 0, pltpu.roll(v, step, 0), pltpu.roll(v, SUBLANES - step, 0))

        def body(g):
            for i in range(GROUP):
                i = g * GROUP + i
                amps = []
                for v in range(per):
                    re, im = take(buf, k, i, rows(v))
                    for step in (1, 2, 4):
                        pr, pi = partner(re, step), partner(im, step)
                        re, im = c * re + s * pi, c * im - s * pr
                    amps.append((re, im))
                for v, amp in enumerate(rx_list(amps, c, s)):
                    keep(buf, k, i, rows(v), amp)

        loop(0, BLOCKS // GROUP, body)

    def block_bits(l, k, get, dst):
        c, s = tabs[l, 0], tabs[l, 1]
        for v in range(per):
            amps = rx_list([get(i, rows(v)) for i in range(BLOCKS)], c, s)
            for i, amp in enumerate(amps):
                keep(dst, k, i, rows(v), amp)

    def chunk_pair(k0, k1, l):
        c, s = tabs[l, 0], tabs[l, 1]

        def body(i):
            for v in range(per):
                p0, p1 = rx_pair(take(work, k0, i, rows(v)), take(work, k1, i, rows(v)), c, s)
                keep(work, k0, i, rows(v), p0)
                keep(work, k1, i, rows(v), p1)

        loop(0, BLOCKS, body)

    def ship(group, p):
        lo, size = group
        part = pl.ds(lo, size)
        at = GROUPS.index(group)

        for j, dev in peers:
            put(send.at[p, j, part], recv.at[p, me, part], send_sem.at[p, at], recv_sem.at[p, at], dev).start()
        recv[p, me, part] = send[p, me, part]

    def sent(p):
        for at, (lo, size) in enumerate(GROUPS):
            part = send.at[p, pl.ds(0, BLOCKS - 1), pl.ds(lo, size)]
            pltpu.make_async_copy(part, part, send_sem.at[p, at]).wait()

    def arrived(group, p):
        lo, size = group
        part = recv.at[p, pl.ds(0, BLOCKS - 1), pl.ds(lo, size)]
        pltpu.make_async_copy(part, part, recv_sem.at[p, GROUPS.index(group)]).wait()

    def phased(k, get):
        def phased_get(i, r):
            (re, im), (co, si) = get(i, r), take(trig, k, i, r)
            return re * co + im * si, im * co - re * si

        return phased_get

    def collect(l, p):
        def fetch(k):
            block_bits(l, k, lambda i, r: take(recv.at[p], k, i, r), work)

        def early(k):
            fetch(k)
            inner(work, k, l)

        for group in GROUPS:
            lo, size = group
            hi = lo + size
            if lo in (0, half):
                pl.when(l < layers - 1)(
                    lambda: loop(lo, lo + half, lambda k: angles(l + 1, cost.at[1 - p], trig, k)))
            arrived(group, p)
            loop(lo, hi, early if hi <= half else fetch)
            if hi < n:
                chunk_pair(lo, lo + 1, l)
            if hi == half:
                loop(0, 2, lambda i: chunk_pair(i, i + 2, l))

    def first_chunk(l, k):
        c, s = tabs[l, 0], tabs[l, 1]

        def get(i, r):
            upper = rx_pair(take(work, 6 + k, i, r), take(work, 7 - k, i, r), c, s)[0]
            upper = rx_pair(take(work, 4 + k, i, r), upper, c, s)[0]
            return rx_pair(take(work, k, i, r), upper, c, s)[0]

        return get

    def rest(l):
        chunk_pair(6, 7, l)
        loop(0, 2, lambda i: chunk_pair(4 + i, 6 + i, l))

    def first(trig_ref, k):
        return lambda i, r: (trig_ref[i, k, 0, r, :], -trig_ref[i, k, 1, r, :])

    def start(k, targets):
        if targets is peers:
            pl.semaphore_wait(ready_sem, len(near))
            for j, dev in peers[:8]:
                put(cost.at[0, j, k], cost.at[1, me, k], csend_sem, crecv_sem.at[k], dev).start()
        angles(0, cost.at[0], trig, k)
        block_bits(0, k, first(trig, k), send.at[0])
        if targets is peers:
            inner(send.at[0], k, 0)
        for j, dev in targets:
            put(send.at[0, j, k], recv.at[0, me, k], fsend_sem.at[k], frecv_sem.at[k], dev).start()
        recv[0, me, k] = send[0, me, k]

    def proxy(k):
        both = pl.ds(a * 4 + 2 * (1 - half_z), 2)
        for x in range(2):
            pltpu.make_async_copy(far_cost.at[x, :, k], far_cost.at[x, :, k], xrecv_sem.at[x, k]).wait()
        for j, dev in near:
            put(far_cost.at[:, j, k], cost.at[1, both, k], pcsend_sem, crecv_sem.at[k], dev).start()
        pltpu.make_async_copy(far_cost.at[:, me, k], cost.at[1, both, k], crecv_sem.at[k]).start()

        def one(x):
            angles(0, far_cost.at[x], far_send.at[x], k)
            block_bits(0, k, first(far_send.at[x], k), far_send.at[x])

        loop(0, 2, one)
        for j, dev in near:
            put(far_send.at[:, j, k], recv.at[0, both, k], psend_sem.at[k], frecv_sem.at[k], dev).start()
        pltpu.make_async_copy(far_send.at[:, me, k], recv.at[0, both, k], frecv_sem.at[k]).start()

    def first_collect(k, last=False):
        part = cost.at[0, pl.ds(0, 8), k]
        pltpu.make_async_copy(part, part, crecv_sem.at[k]).wait()
        angles(1, cost.at[1], trig, k)
        if last:
            chunk_pair(4, 5, 0)
            loop(0, 2, lambda i: chunk_pair(2 * i, 2 * i + 1, 0))
            loop(0, 2, lambda i: chunk_pair(i, i + 2, 0))
        part = recv.at[0, pl.ds(0, BLOCKS - 1), k]
        pltpu.make_async_copy(part, part, frecv_sem.at[k]).wait()
        block_bits(0, k, lambda i, r: take(recv.at[0], k, i, r), work)
        if not last:
            inner(work, k, 0)

    def begin(k):
        start(k, near)
        pl.when(k < n - 2)(lambda: cross(k + 1).start())

    loop(0, n - 1, begin)
    start(n - 1, peers)

    def step(k):
        pl.when(proxy_role)(lambda: proxy(k))

        @pl.when(k == 1)
        def _():
            part = cost.at[0, pl.ds(0, len(near))]
            pltpu.make_async_copy(part, part, nrecv_sem).wait()

        pl.when(k > 0)(lambda: first_collect(k - 1))

    loop(0, n - 1, step)
    first_collect(n - 2)
    first_collect(n - 1, True)

    def first_sent(k):
        pltpu.make_async_copy(cost.at[0, :, k], cost.at[0, :, k], xsend_sem.at[k]).wait()
        part = send.at[0, pl.ds(0, len(near)), k]
        pltpu.make_async_copy(part, part, fsend_sem.at[k]).wait()

    def first_sends():
        loop(0, n - 1, first_sent)
        part = send.at[0, pl.ds(0, len(peers)), n - 1]
        pltpu.make_async_copy(part, part, fsend_sem.at[n - 1]).wait()
        part = cost.at[0, pl.ds(0, (len(near) * (n - 1) + len(peers)) // n)]
        pltpu.make_async_copy(part, part, csend_sem).wait()

        @pl.when(proxy_role)
        def _():
            part = cost.at[0, pl.ds(0, 2 * len(near)), pl.ds(0, n - 1)]
            pltpu.make_async_copy(part, part, pcsend_sem).wait()

            def one(k):
                part = recv.at[0, pl.ds(0, 2 * len(near)), k]
                pltpu.make_async_copy(part, part, psend_sem.at[k]).wait()

            loop(0, n - 1, one)

    def layer(l):
        p = l % 2
        pl.when(l == 1)(first_sends)
        pl.when(l > 1)(lambda: sent(1 - p))
        for group in GROUPS:
            lo, size = group
            if lo == 0:
                loop(0, 2, lambda k: block_bits(l + 1, k, phased(k, first_chunk(l, k)), send.at[1 - p]))
                ship(group, 1 - p)
                rest(l)
                loop(0, half, lambda k: chunk_pair(k, k + half, l))
                continue

            def resend(k):
                block_bits(l + 1, k, phased(k, lambda i, r: take(work, k, i, r)), send.at[1 - p])
                if lo >= half:
                    inner(send.at[1 - p], k, l + 1)

            loop(lo, lo + size, resend)
            ship(group, 1 - p)
        collect(l + 1, 1 - p)

    loop(0, layers - 1, layer)

    last = layers - 1
    c, s = tabs[last, 0], tabs[last, 1]

    def finish(i, acc):
        for v in range(per):
            r = rows(v)
            amps = [take(work, k, i, r) for k in range(n)]
            for k0, k1 in ((6, 7), (4, 6), (5, 7), (0, 4), (1, 5), (2, 6), (3, 7)):
                amps[k0], amps[k1] = rx_pair(amps[k0], amps[k1], c, s)
            for k, (re, im) in enumerate(amps):
                keep(work, k, i, r, (re, im))
                acc = acc + cost[0, i, k, r, :] * (re * re + im * im)
        return acc

    en_send[...] = lax.fori_loop(0, BLOCKS, finish, jnp.zeros((SUBLANES, LANES), jnp.float32))
    for _, dev in peers:
        put(en_send, en_recv.at[me], esend_sem, erecv_sem, dev).start()
    en_recv[me] = en_send[...]
    part = en_recv.at[pl.ds(0, BLOCKS - 1)]
    sent(1 - last % 2)
    sent(last % 2)
    pltpu.make_async_copy(part, part, erecv_sem).wait()
    pltpu.make_async_copy(part, part, esend_sem).wait()
    full = en_recv[0]
    for i in range(1, BLOCKS):
        full = full + en_recv[i]
    en_out[0] = jnp.sum(full) / total


def split_kernel(pair, re_out, im_out, sem):
    copies = [pltpu.make_async_copy(pair.at[part], out, sem.at[part])
              for part, out in enumerate((re_out, im_out))]
    for copy in copies:
        copy.start()
    for copy in copies:
        copy.wait()


def solution(mesh):
    state_spec = P(("inst", "qx", "qy"))

    def device_body(cost_local, gammas, betas):
        local = cost_local.shape[0]
        vregs = local // (BLOCKS * SUBLANES * LANES)
        layers = gammas.shape[0]
        n = CHUNKS
        r = vregs // n * SUBLANES
        shape = (BLOCKS, n, r, LANES)
        pair = (BLOCKS, n, 2, r, LANES)
        f32 = jnp.float32
        any_spec = pl.BlockSpec(memory_space=pl.ANY)
        smem = pl.BlockSpec(memory_space=pltpu.SMEM)
        vmem = pl.BlockSpec(memory_space=pltpu.VMEM)
        dma = pltpu.SemaphoreType.DMA
        g = len(GROUPS)
        energy, state = pl.pallas_call(
            functools.partial(kernel, layers, vregs, float(local * BLOCKS)),
            out_shape=[jax.ShapeDtypeStruct((1,), f32), pltpu.VMEM((2,) + shape, f32)],
            in_specs=[any_spec, smem, smem],
            out_specs=[smem, vmem],
            scratch_shapes=[
                pltpu.VMEM((2,) + shape, f32),
                pltpu.VMEM(pair, f32),
                pltpu.VMEM((2,) + pair, f32),
                pltpu.VMEM((2,) + pair, f32),
                pltpu.VMEM((layers, 2 * LANES, 2 * LANES), f32),
                pltpu.VMEM((layers, 2, SUBLANES, LANES), f32),
                pltpu.VMEM((SUBLANES, LANES), f32),
                pltpu.VMEM((BLOCKS, SUBLANES, LANES), f32),
                pltpu.VMEM((2,) + shape, f32),
                pltpu.VMEM((2,) + pair, f32),
                dma, dma, dma((n,)), dma((2, g)), dma((2, g)), dma, dma,
                dma((n,)), dma((n,)), dma((n,)), dma((2, n)), dma, dma((n,)), dma,
                pltpu.SemaphoreType.REGULAR,
            ],
            compiler_params=pltpu.CompilerParams(collective_id=0, has_side_effects=True),
            name="qaoa",
        )(cost_local.reshape(shape), gammas, betas)
        out_re, out_im = pl.pallas_call(
            split_kernel,
            out_shape=[jax.ShapeDtypeStruct(shape, f32)] * 2,
            in_specs=[vmem],
            out_specs=[any_spec] * 2,
            scratch_shapes=[dma((2,))],
            name="split",
        )(pltpu.with_memory_space_constraint(state, pltpu.VMEM))
        return energy, out_re.reshape(local), out_im.reshape(local)

    return jax.shard_map(device_body, mesh=mesh, in_specs=(state_spec, P(), P()),
                         out_specs=(P("inst"), state_spec, state_spec), check_vma=False)
```
